128 devices in a mesh: rep: 2 (over core), dp: 64 (over x, y, z).
Axes of the slice: x: 4, y: 4, z: 4, core: 2. Of those that a mesh axis runs over, the one named last changes fastest.
Arguments:
- x: bfloat16 [128, 2048, 768], P(('rep', 'dp')), parts along dimension 0
- dy: bfloat16 [128, 2048, 768], P(('rep', 'dp')), parts along dimension 0
- w_gate: bfloat16 [2, 768, 3072], replicated
- w_up: bfloat16 [2, 768, 3072], replicated
- w_down: bfloat16 [2, 3072, 768], replicated
- m_w_gate: float32 [2, 768, 3072], replicated
- m_w_up: float32 [2, 768, 3072], replicated
- m_w_down: float32 [2, 3072, 768], replicated
- v_w_gate: float32 [2, 768, 3072], replicated
- v_w_up: float32 [2, 768, 3072], replicated
- v_w_down: float32 [2, 3072, 768], replicated
Outputs:
- output 1: bfloat16 [4, 768, 3072], P('rep'), parts along dimension 0
- output 2: bfloat16 [4, 768, 3072], P('rep'), parts along dimension 0
- output 3: bfloat16 [4, 3072, 768], P('rep'), parts along dimension 0
- output 4: float32 [4, 768, 3072], P('rep'), parts along dimension 0
- output 5: float32 [4, 768, 3072], P('rep'), parts along dimension 0
- output 6: float32 [4, 3072, 768], P('rep'), parts along dimension 0
- output 7: float32 [4, 768, 3072], P('rep'), parts along dimension 0
- output 8: float32 [4, 768, 3072], P('rep'), parts along dimension 0
- output 9: float32 [4, 3072, 768], P('rep'), parts along dimension 0
There are 2 independent parts. The reference program is written for one: setup_inputs(seed, part) draws one part's arguments, and reference() takes and returns one part's arrays. A program takes and returns all parts, laid end to end along the dimension named above; an argument that names none is the same for every part.
All inputs are finite; a program needn't handle non-finite values.
Results may differ from the reference program's by a relative error of at most 0.022.
Values are sent between devices in bfloat16 or wider.
A program may use at most 1.5 GiB of HBM per device.

```python
import jax
import jax.numpy as jnp
from jax import lax

SEQUENCES = 64
TOKENS = 2048
D = 768
FF = 3072
LAYERS = 2
NAMES = ("w_gate", "w_up", "w_down")
SHAPES = {"w_gate": (LAYERS, D, FF), "w_up": (LAYERS, D, FF), "w_down": (LAYERS, FF, D)}


def bump(key, n, height):
    away = (jnp.arange(n, dtype=jnp.int32) - jax.random.randint(key, (), 0, n, jnp.int32)) % n
    return jnp.where(away < n // 8, height, 1.0)


def together(key, own, strength):
    shared = jax.random.normal(key, own.shape[1:], jnp.float32)
    return (own + strength * shared) * lax.rsqrt(1 + strength * strength)


def setup_inputs(seed: int = 0, part: int = 0) -> dict:
    kx, kdy, ka, kb, kz, kf, kh, kl, *keys = jax.random.split(jax.random.key(seed), 8 + 3 * len(NAMES))
    kx, kdy, ka, kb = (jax.random.fold_in(k, part) for k in (kx, kdy, ka, kb))
    kw, km, kv = (keys[i::3] for i in range(3))
    shape = (SEQUENCES, TOKENS, D)
    much_x, much_dy = jax.random.uniform(kz, (2,), jnp.float32, 0.0, 1.0)
    loud = 2.0 ** jax.random.uniform(jax.random.fold_in(kz, 1), (), jnp.float32, -1.0, 2.0)
    layers = 2.0 ** jax.random.uniform(kl, (LAYERS, 1, 1), jnp.float32, -1.0, 1.0)
    x = together(ka, jax.random.normal(kx, shape, jnp.float32), much_x) * bump(kf, D, 4.0)
    dy = together(kb, jax.random.normal(kdy, shape, jnp.float32), much_dy)
    drawn = {"x": x.astype(jnp.bfloat16), "dy": (loud * dy * (SEQUENCES * TOKENS) ** -0.5).astype(jnp.bfloat16)}
    for key, name in zip(kw, NAMES, strict=True):
        w = jax.random.normal(key, SHAPES[name], jnp.float32) * SHAPES[name][1] ** -0.5
        drawn[name] = (w * {"w_gate": 1.0, "w_up": bump(kh, FF, 4.0), "w_down": layers}[name]).astype(jnp.bfloat16)
    for key, name in zip(km, NAMES, strict=True):
        drawn[f"m_{name}"] = 0.1 * jax.random.normal(key, SHAPES[name], jnp.float32)
    for key, name in zip(kv, NAMES, strict=True):
        drawn[f"v_{name}"] = jax.random.uniform(key, SHAPES[name], jnp.float32, 0.005, 0.015)
    return drawn


def matmul(a, w):
    return jnp.dot(a, w, preferred_element_type=jnp.float32).astype(jnp.bfloat16)


def normed(h):
    wide = h.astype(jnp.float32)
    scale = lax.rsqrt(jnp.mean(wide**2, -1, keepdims=True) + 1e-6)
    return (wide * scale).astype(jnp.bfloat16)


def layer(h, w):
    a = normed(h)
    gate = jnp.dot(a, w["w_gate"], preferred_element_type=jnp.float32)
    up = jnp.dot(a, w["w_up"], preferred_element_type=jnp.float32)
    return h + matmul((jax.nn.silu(gate) * up).astype(jnp.bfloat16), w["w_down"])


def adamw(w, m, v, g):
    m = 0.9 * m + 0.1 * g
    v = 0.95 * v + 0.05 * g * g
    step = m * lax.rsqrt(v + 1e-8) + 0.1 * w
    return (w - 0.02 * step).astype(jnp.bfloat16), m, v


def clipped(gradients, sum_of_squares, count):
    factor = jnp.minimum(1.0, 0.5 * lax.rsqrt(sum_of_squares / count + 1e-30))
    return [g * factor for g in gradients]


def stack(weights, h):
    return lax.scan(lambda h, w: (layer(h, w), None), h, weights)[0]


def reference(x, dy, w_gate, w_up, w_down, m_w_gate, m_w_up, m_w_down, v_w_gate, v_w_up, v_w_down):
    weights = dict(zip(NAMES, (w_gate, w_up, w_down), strict=True))

    def take(so_far, sequence):
        h, by_y = sequence
        _, back = jax.vjp(lambda w: stack(w, h), weights)
        return jax.tree.map(lambda total, term: total + term.astype(jnp.float32), so_far, back(by_y)[0]), None

    none_yet = {name: jnp.zeros(w.shape, jnp.float32) for name, w in weights.items()}
    by_weights, _ = lax.scan(take, none_yet, (x, dy))
    gradients = [by_weights[name].astype(jnp.bfloat16).astype(jnp.float32) for name in NAMES]
    gradients = clipped(gradients, sum(jnp.sum(g * g) for g in gradients), sum(g.size for g in gradients))
    new = [
        adamw(w.astype(jnp.float32), m, v, g)
        for w, m, v, g in zip((w_gate, w_up, w_down), (m_w_gate, m_w_up, m_w_down), (v_w_gate, v_w_up, v_w_down), gradients, strict=True)
    ]
    return tuple(one[which] for which in range(3) for one in new)
```

```python
import functools

import jax
import jax.numpy as jnp
from jax import lax
from jax.experimental import pallas as pl
from jax.experimental.pallas import tpu as pltpu
from jax.sharding import PartitionSpec as P

f32, bf16 = jnp.float32, jnp.bfloat16
MESH = pl.DeviceIdType.MESH
SIDE = 4
STRIDE = (16, 4, 1)
COLS = 512
ROWS = 512
HIGH, WIDE = 48, 128
AHEAD = 4
VMEM_LIMIT = 66_900_000


def nn(a, b):
    return jnp.dot(a, b, preferred_element_type=f32)


def nt(a, b):
    return lax.dot_general(a, b, (((1,), (1,)), ((), ())), preferred_element_type=f32)


def scale_of(wide):
    return lax.rsqrt(jnp.mean(wide * wide, -1, keepdims=True) + 1e-6)


def normed(h):
    wide = h.astype(f32)
    return (wide * scale_of(wide)).astype(bf16)


def gates(gate, up):
    sig = 1.0 / (1.0 + jnp.exp(-gate))
    return gate * sig, up * (sig * (1.0 + gate * (1.0 - sig)))


def rows_loop(tokens, body, step=256):
    def one(c, _):
        body(pl.ds(pl.multiple_of(c * step, step), step))
        return 0

    lax.fori_loop(0, tokens // step, one, 0)


def forward_kernel(n_blocks, x_ref, wg, wu, wd, h_ref, p_ref, q_ref, act_ref, a_s, acc_s):
    block = pl.program_id(0)
    tokens = x_ref.shape[0]

    @pl.when(block == 0)
    def _():
        def body(r):
            a_s[r, :] = normed(x_ref[r, :])
            acc_s[r, :] = jnp.zeros((256, acc_s.shape[1]), f32)

        rows_loop(tokens, body)

    for c in range(tokens // ROWS):
        r = pl.ds(c * ROWS, ROWS)
        a = a_s[r, :]
        gate, up = nn(a, wg[0]), nn(a, wu[0])
        q, p = gates(gate, up)
        p_ref[r, :] = p
        q_ref[r, :] = q
        act = (q * up).astype(bf16)
        act_ref[r, :] = act
        acc_s[r, :] += nn(act, wd[0])

    @pl.when(block == n_blocks - 1)
    def _():
        def body(r):
            h_ref[r, :] = (x_ref[r, :].astype(f32) + acc_s[r, :].astype(bf16).astype(f32)).astype(bf16)

        rows_loop(tokens, body)


def forward(x, wg, wu, wd):
    tokens, d = x.shape
    ff = wg.shape[2]
    n_blocks = ff // COLS
    whole = pl.BlockSpec((tokens, d), lambda b: (0, 0))
    wide = pl.BlockSpec((1, d, COLS), lambda b: (0, 0, b))
    hidden = pl.BlockSpec((tokens, COLS), lambda b: (0, b))
    return pl.pallas_call(
        functools.partial(forward_kernel, n_blocks),
        grid=(n_blocks,),
        out_shape=(
            jax.ShapeDtypeStruct((tokens, d), bf16),
            jax.ShapeDtypeStruct((tokens, ff), f32),
            jax.ShapeDtypeStruct((tokens, ff), f32),
            jax.ShapeDtypeStruct((tokens, ff), bf16),
        ),
        in_specs=[whole, wide, wide, pl.BlockSpec((1, COLS, d), lambda b: (0, b, 0))],
        out_specs=(whole, hidden, hidden, hidden),
        scratch_shapes=[pltpu.VMEM((tokens, d), bf16), pltpu.VMEM((tokens, d), f32)],
        compiler_params=pltpu.CompilerParams(vmem_limit_bytes=VMEM_LIMIT),
        cost_estimate=pl.CostEstimate(flops=6 * tokens * d * ff, bytes_accessed=10 * tokens * ff, transcendentals=0),
        name="forward",
    )(x, wg, wu, wd)


def dims_of(k):
    return k, (k + 1) % 3, (k + 2) % 3


def backward_kernel(n_blocks, count, x_ref, dy_ref, h_ref, p_ref, q_ref, act_ref, wg, wu, wd, *refs):
    outs, factor_ref = (refs[0:3], refs[3:6]), refs[6]
    (
        a_s, aT_s, dy_s, dyT_s, h_s, acc_s, wg_s, wu_s, wd_s, act_s, dg_s, du_s, p_s, q_s,
        own, f1, b2, f2, b3, ag, ssq, nrm,
        through1, through2, straight1, straight2, passed1, passed2, sums1, sums2, r3,
        w_sem, in_sem, pq_sem, act_sem, own_sem,
        snd1, snd2, rcv1, rcv2, s3_snd, s3_rcv, g1_snd, g1_rcv, g2_snd, g2_rcv, n_snd, n_rcv,
    ) = refs[7:]
    tokens, d = dy_s.shape
    steps = 2 * n_blocks
    me = lax.axis_index("dp")
    at = tuple(me // s % SIDE for s in STRIDE)
    offsets = (1, 3, 2)

    def to(dim, s):
        return {"dp": me + ((at[dim] + s) % SIDE - at[dim]) * STRIDE[dim]}

    def send(src, dst, snd, rcv, dim, s):
        return pltpu.make_async_remote_copy(src_ref=src, dst_ref=dst, send_sem=snd, recv_sem=rcv, device_id=to(dim, s), device_id_type=MESH)

    barrier = pltpu.get_barrier_semaphore()
    for dim in range(3):
        for s in offsets:
            pl.semaphore_signal(barrier, inc=1, device_id=to(dim, s), device_id_type=MESH)

    def columns(i):
        return pl.ds(pl.multiple_of(i * COLS, COLS), COLS)

    def load_up(i, slot):
        pairs = ((wg, wg_s), (wu, wu_s))
        return [pltpu.make_async_copy(w.at[1, :, columns(i)], to.at[slot], w_sem.at[slot, n]) for n, (w, to) in enumerate(pairs)]

    def load_down(layer, i, slot):
        return pltpu.make_async_copy(wd.at[layer, columns(i), :], wd_s.at[slot], w_sem.at[slot, 2])

    def load_pq(i):
        pairs = ((p_ref, p_s), (q_ref, q_s))
        return [pltpu.make_async_copy(src.at[:, columns(i)], to, pq_sem.at[n]) for n, (src, to) in enumerate(pairs)]

    def load_act(i):
        return pltpu.make_async_copy(act_ref.at[:, columns(i)], act_s, act_sem)

    def start(copies):
        for c in copies:
            c.start()

    def wait(copies):
        for c in copies:
            c.wait()

    load_h = pltpu.make_async_copy(h_ref, h_s, in_sem.at[0])
    load_dy = pltpu.make_async_copy(dy_ref, dy_s, in_sem.at[1])
    load_x = pltpu.make_async_copy(x_ref, a_s, in_sem.at[2])
    start([load_h, load_dy, *load_up(0, 0), load_down(1, 0, 0), *load_pq(0)])
    ssq[...] = jnp.zeros_like(ssq)
    wait([load_h, load_dy])

    def begin(r):
        a = normed(h_s[r, :])
        a_s[r, :] = a
        aT_s[:, r] = a.T
        dyT_s[:, r] = dy_s[r, :].T
        acc_s[r, :] = jnp.zeros((r.size, d), f32)

    rows_loop(tokens, begin)
    pl.semaphore_wait(barrier, 9)

    def second_layer(i):
        slot = i % 2
        wait([*load_up(i, slot), load_down(1, i, slot)])

        @pl.when(i < n_blocks - 1)
        def _():
            start([*load_up(i + 1, 1 - slot), load_down(1, i + 1, 1 - slot)])

        @pl.when(i == n_blocks - 1)
        def _():
            load_down(0, 0, 1 - slot).start()

        for c in range(tokens // ROWS):
            r = pl.ds(c * ROWS, ROWS)
            a = a_s[r, :]
            gate, up = nn(a, wg_s[slot]), nn(a, wu_s[slot])
            by_act = nt(dy_s[r, :], wd_s[slot]).astype(bf16).astype(f32)
            q, p = gates(gate, up)
            act_s[r, :] = (q * up).astype(bf16)
            by_gate, by_up = (by_act * p).astype(bf16), (by_act * q).astype(bf16)
            dg_s[r, :] = by_gate
            du_s[r, :] = by_up
            acc_s[r, :] += nt(by_gate, wg_s[slot]) + nt(by_up, wu_s[slot])

    def between():
        load_x.start()

        def back(r):
            wide = h_s[r, :].astype(f32)
            s = scale_of(wide)
            by_a = acc_s[r, :].astype(bf16).astype(f32)
            along = jnp.sum(by_a * wide, -1, keepdims=True)
            by_h = (by_a * s - wide * (s * s * s * along * (1.0 / d))).astype(bf16)
            total = (dy_s[r, :].astype(f32) + by_h.astype(f32)).astype(bf16)
            dy_s[r, :] = total
            dyT_s[:, r] = total.T

        rows_loop(tokens, back)
        load_x.wait()

        def again(r):
            aT_s[:, r] = normed(a_s[r, :]).T

        rows_loop(tokens, again)

    def first_layer(i, block):
        slot = i % 2
        load_act(block).start()
        wait([load_down(0, block, slot), *load_pq(block)])

        @pl.when(block < n_blocks - 1)
        def _():
            load_down(0, block + 1, 1 - slot).start()

        for c in range(tokens // ROWS):
            r = pl.ds(c * ROWS, ROWS)
            by_act = nt(dy_s[r, :], wd_s[slot]).astype(bf16).astype(f32)
            dg_s[r, :] = (by_act * p_s[r, :]).astype(bf16)
            du_s[r, :] = (by_act * q_s[r, :]).astype(bf16)

        @pl.when(block < n_blocks - 1)
        def _():
            start(load_pq(block + 1))

        load_act(block).wait()

    def weight_gradient(slot, k):
        if k < 2:
            g = nn(aT_s[...], (dg_s, du_s)[k][...]).astype(bf16)
        else:
            g = nn(dyT_s[...], act_s[...]).astype(bf16)
        for p in range(SIDE):
            for q in range(SIDE):
                for r in range(SIDE):
                    row, col = ((p * SIDE + q), r) if k < 2 else ((q * SIDE + r), p)
                    own[slot, k, p, q, r] = g[row * HIGH : row * HIGH + HIGH, col * WIDE : col * WIDE + WIDE]

    stages = (
        (through1, straight1, passed1, sums1, snd1, rcv1),
        (through2, straight2, passed2, sums2, snd2, rcv2),
    )

    def piece(stage, j, k, whose, half):
        part = pl.ds(half * 2, 2)
        return b2.at[k, whose, part] if stage else own.at[j % 2, k, whose, part]

    def around(stage, k):
        c = at[dims_of(k)[stage]]
        return (c + 1) % SIDE, (c + 3) % SIDE, (c + 2) % SIDE

    def sends(stage, kind, j, k):
        buffers, snd, rcv = stages[stage][:3], stages[stage][-2], stages[stage][-1]
        nxt, prv, far = around(stage, k)
        slot = j % buffers[kind].shape[0]
        copies = []
        for half in range(2):
            down = half == 0 if kind != 1 else half == 1
            src = stages[stage][3].at[k, half] if kind == 2 else piece(stage, j, k, (nxt, prv)[half] if kind else far, half)
            copies.append(
                send(src, buffers[kind].at[slot, k, half], snd.at[kind, j % 2, k, half], rcv.at[kind, slot, k, half], dims_of(k)[stage], 3 if down else 1)
            )
        return copies

    def pass_on(stage, j):
        through, sums = stages[stage][0], stages[stage][3]
        slot = j % 2
        for k in range(3):
            nxt, prv, _ = around(stage, k)
            onward = sends(stage, 2, j, k)
            for c in sends(stage, 0, j, k):
                c.wait_recv()
            for half, whose in enumerate((prv, nxt)):
                for q in range(2):
                    if stage:
                        sums[k, half, q] = (through[slot, k, half, q].astype(f32) + f1[k, whose, half * 2 + q]).astype(bf16)
                    else:
                        for r in range(SIDE):
                            mine = own[slot, k, whose, half * 2 + q, r].astype(f32)
                            sums[k, half, q, r] = (through[slot, k, half, q, r].astype(f32) + mine).astype(bf16)
                onward[half].start()
        if stage:
            done_sending(stage, (0, 1), j)

    def done_sending(stage, kinds, j):
        for k in range(3):
            for kind in kinds:
                for c in sends(stage, kind, j, k):
                    c.wait_send()

    def sum_1(j):
        slot, far_slot = j % 2, j % straight1.shape[0]
        for k in range(3):
            c = at[dims_of(k)[0]]
            for half in range(2):
                sends(0, 1, j, k)[half].wait_recv()
                sends(0, 2, j, k)[half].wait_recv()
                for q in range(2):
                    for r in range(SIDE):
                        total = own[slot, k, c, half * 2 + q, r].astype(f32) + passed1[slot, k, half, q, r].astype(f32)
                        total = total + straight1[far_slot, k, half, q, r].astype(f32)
                        f1[k, half * 2 + q, r] = total
                        b2[k, half * 2 + q, r] = total.astype(bf16)
            start(sends(1, 0, j, k) + sends(1, 1, j, k))
        done_sending(0, range(3), j)

    def sum_2(j):
        slot = j % 2
        for k in range(3):
            c = at[dims_of(k)[1]]
            for half in range(2):
                sends(1, 1, j, k)[half].wait_recv()
                sends(1, 2, j, k)[half].wait_recv()
                for q in range(2):
                    total = f1[k, c, half * 2 + q] + passed2[slot, k, half, q].astype(f32) + straight2[slot, k, half, q].astype(f32)
                    f2[k, half * 2 + q] = total
                    b3[k, half * 2 + q] = total.astype(bf16)
            start(sends_3(slot, k))
        done_sending(1, (2,), j)

    def sends_3(slot, k):
        r = dims_of(k)[2]
        return [send(b3.at[k, (at[r] + s) % SIDE], r3.at[slot, k, s - 1], s3_snd.at[k, s - 1], s3_rcv.at[slot, k, s - 1], r, s) for s in offsets]

    def sends_g1(slot, k):
        r = dims_of(k)[2]
        mine = ag.at[slot, k, at[r]]
        return [send(mine, mine, g1_snd.at[k, s - 1], g1_rcv.at[slot, k, s - 1], r, s) for s in offsets]

    def sum_3(j):
        slot = j % 2
        for k in range(3):
            for c in sends_3(slot, k):
                c.wait_recv()
            total = f2[k, at[dims_of(k)[2]]]
            for s in range(3):
                total = total + r3[slot, k, s].astype(f32)
            g = total.astype(bf16)
            ag[slot, k, at[dims_of(k)[2]]] = g
            start(sends_g1(slot, k))
            wide = g.astype(f32)
            wide = wide * wide
            for row in range(0, HIGH, 8):
                ssq[...] += wide[row : row + 8]
        for k in range(3):
            for c in sends_3(slot, k):
                c.wait_send()

    def by_half(j, do):
        @pl.when(j < n_blocks)
        def _():
            do(j, outs[0])

        @pl.when(j >= n_blocks)
        def _():
            do(j - n_blocks, outs[1])

    def sends_g2(j, block, out, k):
        q = dims_of(k)[1]
        mine = ag.at[j % 2, k]
        return [send(mine, out[k].at[block, at[q]], g2_snd.at[0, k, way], g2_rcv.at[0, j, k, way], q, s) for way, s in enumerate((1, 3))]

    def keep_g2(j, block, out, k):
        return pltpu.make_async_copy(ag.at[j % 2, k], out[k].at[block, at[dims_of(k)[1]]], own_sem.at[k])

    def sends_g3(j, block, out, k):
        q = dims_of(k)[1]
        copies = []
        for way, s in enumerate((1, 3)):
            part = out[k].at[block, (at[q] + SIDE - s) % SIDE, pl.ds(way * 2, 2)]
            copies.append(send(part, part, g2_snd.at[1, k, way], g2_rcv.at[1, j, k, way], q, s))
        return copies

    def share(j):
        for k in range(3):
            for c in sends_g1(j % 2, k):
                c.wait_recv()
                c.wait_send()

        def do(block, out):
            for k in range(3):
                start(sends_g2(j, block, out, k) + [keep_g2(j, block, out, k)])

        by_half(j, do)

    def share_on(j):
        def do(block, out):
            for k in range(3):
                for there, on in zip(sends_g2(j, block, out, k), sends_g3(j, block, out, k), strict=True):
                    there.wait_recv()
                    on.start()
            for k in range(3):
                for c in sends_g2(j, block, out, k):
                    c.wait_send()
                keep_g2(j, block, out, k).wait()

        by_half(j, do)

    def shared(j):
        def do(block, out):
            for k in range(3):
                for c in sends_g3(j, block, out, k):
                    c.wait()

        by_half(j, do)

    def sends_n(stage):
        mine = nrm.at[stage, at[stage]]
        return [send(mine, mine, n_snd.at[stage, s - 1], n_rcv.at[stage, s - 1], stage, s) for s in offsets]

    def norm_send(stage, value):
        nrm[stage, at[stage]] = value
        start(sends_n(stage))

    def norm_take(stage):
        wait(sends_n(stage))
        total = nrm[stage, 0]
        for s in range(1, SIDE):
            total = total + nrm[stage, s]
        return total

    def when(i, lag, do, *args):
        pl.when((i >= lag) & (i < steps + lag))(lambda: do(*args, i - lag))

    def step(i, _):
        @pl.when(i < n_blocks)
        def _():
            second_layer(i)

        @pl.when(i == n_blocks)
        def _():
            between()

        @pl.when((i >= n_blocks) & (i < steps))
        def _():
            first_layer(i, i - n_blocks)

        when(i, 1, pass_on, 0)
        when(i, 2, pass_on, 1)
        when(i, 3, sum_3)

        @pl.when(i == steps + 2)
        def _():
            norm_send(0, ssq[...])

        @pl.when(i == steps + 3)
        def _():
            norm_send(2, norm_take(1))

        when(i, 5, shared)
        when(i, 4, share_on)

        @pl.when(i < steps)
        def _():
            for k in range(3):
                weight_gradient(i % 2, k)
                start(sends(0, 0, i, k) + sends(0, 1, i, k))

        when(i, 2, sum_2)
        when(i, 1, sum_1)

        @pl.when(i == steps + 2)
        def _():
            norm_send(1, norm_take(0))

        when(i, 3, share)
        return 0

    lax.fori_loop(0, steps + 4, step, 0)
    total = jnp.sum(norm_take(2), keepdims=True)
    factor = jnp.minimum(1.0, 0.5 * lax.rsqrt(total * (1.0 / count) + 1e-30))
    factor_ref[...] = jnp.broadcast_to(factor, factor_ref.shape)
    shared(steps - 1)


def backward(x, dy, h, p, q, act, wg, wu, wd):
    tokens, d = x.shape
    ff = wg.shape[2]
    n_blocks = ff // COLS
    steps = 2 * n_blocks
    anywhere = pl.BlockSpec(memory_space=pl.ANY)
    shard = (HIGH, WIDE)
    quarter = jax.ShapeDtypeStruct((n_blocks, SIDE, SIDE, *shard), bf16)

    def dma(*shape):
        return pltpu.SemaphoreType.DMA(shape)

    def narrow(*shape):
        return pltpu.VMEM(shape, bf16)

    def wide(*shape):
        return pltpu.VMEM(shape, f32)

    halves1, halves2 = (3, 2, 2, SIDE, *shard), (3, 2, 2, *shard)
    return pl.pallas_call(
        functools.partial(backward_kernel, n_blocks, float(6 * d * ff)),
        out_shape=(quarter,) * 6 + (jax.ShapeDtypeStruct((8, 128), f32),),
        in_specs=[anywhere] * 9,
        out_specs=(anywhere,) * 6 + (pl.BlockSpec(memory_space=pltpu.VMEM),),
        scratch_shapes=[
            *(narrow(tokens, d), narrow(d, tokens)) * 2,
            narrow(tokens, d),
            wide(tokens, d),
            *(narrow(2, d, COLS),) * 2,
            narrow(2, COLS, d),
            *(narrow(tokens, COLS),) * 3,
            *(wide(tokens, COLS),) * 2,
            narrow(2, 3, SIDE, SIDE, SIDE, *shard),
            wide(3, SIDE, SIDE, *shard),
            narrow(3, SIDE, SIDE, *shard),
            wide(3, SIDE, *shard),
            narrow(3, SIDE, *shard),
            narrow(2, 3, SIDE, *shard),
            wide(8, 128),
            wide(3, SIDE, 8, 128),
            narrow(2, *halves1),
            narrow(2, *halves2),
            narrow(3, *halves1),
            narrow(2, *halves2),
            narrow(2, *halves1),
            narrow(2, *halves2),
            narrow(*halves1),
            narrow(*halves2),
            narrow(2, 3, 3, *shard),
            dma(2, 3),
            dma(3),
            dma(2),
            dma(),
            dma(3),
            *(dma(3, 2, 3, 2),) * 2,
            *(dma(3, 3, 3, 2),) * 2,
            *(dma(3, 3), dma(2, 3, 3)) * 2,
            dma(2, 3, 2),
            dma(2, steps, 3, 2),
            *(dma(3, 3),) * 2,
        ],
        compiler_params=pltpu.CompilerParams(vmem_limit_bytes=VMEM_LIMIT, collective_id=0, has_side_effects=True),
        cost_estimate=pl.CostEstimate(flops=24 * tokens * d * ff, bytes_accessed=10 * tokens * ff, transcendentals=0),
        name="backward",
    )(x, dy, h, p, q, act, wg, wu, wd)


def adamw_tile(factor, w, m, v, g):
    g = g.astype(f32) * factor
    m = 0.9 * m + 0.1 * g
    v = 0.95 * v + 0.05 * (g * g)
    wide = w.astype(f32)
    return (wide - 0.02 * (m * lax.rsqrt(v + 1e-8) + 0.1 * wide)).astype(bf16), m, v


def adamw_kernel(parts, shifts, n_blocks, factor_ref, *refs):
    n = len(parts)
    refs = list(refs)

    def take(count):
        taken = refs[:count]
        del refs[:count]
        return taken

    grads, arrays = take(3 * n), take(9)
    g_sem, in_sem, out_sem = refs[-3:]
    new, g_s, ins, outs = refs[-33:-24], refs[-24:-21], refs[-21:-12], refs[-12:-3]
    factor = factor_ref[...]
    me = lax.axis_index("dp")
    at = tuple(me // s % SIDE for s in STRIDE)
    steps = n * n_blocks

    def tile(k, i):
        part, block = i // n_blocks, i % n_blocks
        layer, shift = parts[0], shifts[0]
        if n > 1:
            layer, shift = layer + (parts[1] - layer) * part, shift + (shifts[1] - shift) * part
        quarter = (at[k] + shift + SIDE) % SIDE
        rows, cols = ins[k].shape[1:]
        if k < 2:
            return layer, pl.ds(pl.multiple_of(quarter * rows, rows), rows), pl.ds(pl.multiple_of(block * cols, cols), cols)
        row = pl.multiple_of((SIDE * block + quarter) * rows, rows)
        return layer, pl.ds(row, rows), slice(None)

    def loads(k, i):
        slot = i % AHEAD
        return [
            pltpu.make_async_copy(arrays[j].at[tile(k, i)], ins[j].at[slot], in_sem.at[slot, j]) for j in range(k, 9, 3)
        ]

    def load_g(k, i, part):
        slot = i % AHEAD
        return pltpu.make_async_copy(grads[3 * part + k].at[i % n_blocks], g_s[k].at[slot], g_sem.at[slot, k])

    def start(k, i):
        for c in loads(k, i):
            c.start()
        for part in range(n):

            @pl.when(i // n_blocks == part)
            def _():
                load_g(k, i, part).start()

    def stores(k, i):
        slot = i % 2
        return [
            pltpu.make_async_copy(outs[j].at[slot], new[j].at[tile(k, i)], out_sem.at[slot, j]) for j in range(k, 9, 3)
        ]

    def wait(k, i):
        for c in stores(k, i):
            c.wait()

    def first(i, _):
        for k in range(3):
            start(k, i)
        return 0

    lax.fori_loop(0, AHEAD, first, 0)

    def step(i, _):
        slot, out = i % AHEAD, i % 2
        for k in range(3):
            for c in loads(k, i):
                c.wait()
            load_g(k, i, 0).wait()

            @pl.when(i >= 2)
            def _():
                wait(k, i - 2)

            def one(where, g):
                done = adamw_tile(factor[0:1, 0:1], *(ins[j][(slot, *where)] for j in range(k, 9, 3)), g)
                for j, value in zip(range(k, 9, 3), done, strict=True):
                    outs[j][(out, *where)] = value

            if k < 2:
                for q in range(SIDE):
                    for r in range(SIDE):
                        one((pl.ds(q * HIGH, HIGH), pl.ds(r * WIDE, WIDE)), g_s[k][slot, q, r])
            else:
                for lo in range(0, SIDE * SIDE * HIGH, WIDE):
                    pieces = [divmod(e, HIGH) for e in range(lo, lo + WIDE, 16)]
                    rows = [g_s[k][slot, n // SIDE, n % SIDE, pl.ds(row, 16)] for n, row in pieces]
                    one((slice(None), pl.ds(lo, WIDE)), jnp.concatenate(rows, 0).T)
            for c in stores(k, i):
                c.start()

            @pl.when(i + AHEAD < steps)
            def _():
                start(k, i + AHEAD)

        return 0

    lax.fori_loop(0, steps, step, 0)
    for k in range(3):
        wait(k, steps - 2)
        wait(k, steps - 1)


def adamw(parts, shifts, factor, grads, w, m, v, into):
    n, n_blocks = len(parts), grads[0].shape[0]
    d, ff = w[0].shape[1:]
    arrays = list(w) + list(m) + list(v)
    anywhere = pl.BlockSpec(memory_space=pl.ANY)
    tiles = [(d // SIDE, COLS), (d // SIDE, COLS), (COLS // SIDE, d)] * 3
    old = list(into or [])
    return pl.pallas_call(
        functools.partial(adamw_kernel, parts, shifts, n_blocks),
        out_shape=tuple(jax.ShapeDtypeStruct(a.shape, a.dtype) for a in arrays),
        in_specs=[pl.BlockSpec(memory_space=pltpu.VMEM)] + [anywhere] * (len(grads) + 9 + len(old)),
        out_specs=(anywhere,) * 9,
        input_output_aliases={1 + len(grads) + 9 + j: j for j in range(len(old))},
        scratch_shapes=[pltpu.VMEM((AHEAD, *grads[0].shape[1:]), bf16)] * 3
        + [pltpu.VMEM((AHEAD, *t), a.dtype) for t, a in zip(tiles, arrays, strict=True)]
        + [pltpu.VMEM((2, *t), a.dtype) for t, a in zip(tiles, arrays, strict=True)]
        + [pltpu.SemaphoreType.DMA(s) for s in ((AHEAD, 3), (AHEAD, 9), (2, 9))],
        compiler_params=pltpu.CompilerParams(vmem_limit_bytes=VMEM_LIMIT),
        cost_estimate=pl.CostEstimate(flops=n * 45_000_000_000, bytes_accessed=n * 16 * d * ff, transcendentals=0),
        name="adamw",
    )(factor, *grads, *arrays, *old)


def ring(dim, s):
    pairs = []
    for i in range(SIDE**3):
        c = i // STRIDE[dim] % SIDE
        pairs.append((i, i + ((c + s) % SIDE - c) * STRIDE[dim]))
    return pairs


def solution(mesh):
    def step(x, dy, *arrays):
        w, m, v = (arrays[i : i + 3] for i in (0, 3, 6))
        x, dy = x[0], dy[0]
        h, p, q, act = forward(x, *w)
        *quarters, factor = backward(x, dy, h, p, q, act, *w)
        second, first = quarters[0:3], quarters[3:6]

        def shift(parts, s):
            return [lax.ppermute(g, "dp", ring(k, s)) for k, g in enumerate(parts)]

        second_up, second_down = shift(second, 1), shift(second, -1)
        first_up, first_down = shift(first, 1), shift(first, -1)
        new = adamw([1, 0], [0, 0], factor, second + first, w, m, v, None)
        second_up, second_down, new = lax.optimization_barrier((second_up, second_down, new))
        second_far = shift(second_up, 1)
        new = adamw([1, 1], [-1, 1], factor, second_up + second_down, w, m, v, new)
        first_up, first_down, new = lax.optimization_barrier((first_up, first_down, new))
        first_far = shift(first_down, -1)
        new = adamw([0, 0], [-1, 1], factor, first_up + first_down, w, m, v, new)
        second_far, first_far, new = lax.optimization_barrier((second_far, first_far, new))
        new = adamw([1, 0], [2, 2], factor, second_far + first_far, w, m, v, new)
        return tuple(new)

    return jax.shard_map(
        step,
        mesh=mesh,
        in_specs=(P(("rep", "dp"), None, None),) * 2 + (P(None, None, None),) * 9,
        out_specs=(P("rep", None, None),) * 9,
        check_vma=False,
    )
```

```python
import functools

import jax
import jax.numpy as jnp
from jax import lax
from jax.experimental import pallas as pl
from jax.experimental.pallas import tpu as pltpu
from jax.sharding import PartitionSpec as P

f32, bf16 = jnp.float32, jnp.bfloat16
MESH = pl.DeviceIdType.MESH
SIDE = 4
STRIDE = (16, 4, 1)
COLS = 512
ROWS = 512
HIGH, WIDE = 48, 128
AHEAD = 4
VMEM_LIMIT = 66_900_000


def nn(a, b):
    return jnp.dot(a, b, preferred_element_type=f32)


def nt(a, b):
    return lax.dot_general(a, b, (((1,), (1,)), ((), ())), preferred_element_type=f32)


def scale_of(wide):
    return lax.rsqrt(jnp.mean(wide * wide, -1, keepdims=True) + 1e-6)


def normed(h):
    wide = h.astype(f32)
    return (wide * scale_of(wide)).astype(bf16)


def gates(gate, up):
    sig = 1.0 / (1.0 + jnp.exp(-gate))
    return gate * sig, up * (sig * (1.0 + gate * (1.0 - sig)))


def rows_loop(tokens, body, step=256):
    def one(c, _):
        body(pl.ds(pl.multiple_of(c * step, step), step))
        return 0

    lax.fori_loop(0, tokens // step, one, 0)


def forward_kernel(n_blocks, x_ref, dy_ref, wg, wu, wd, h_ref, p_ref, q_ref, act_ref, aT_ref, dyT_ref, a_s, acc_s):
    block = pl.program_id(0)
    tokens = x_ref.shape[0]

    @pl.when(block == 0)
    def _():
        def body(r):
            a_s[r, :] = normed(x_ref[r, :])
            acc_s[r, :] = jnp.zeros((256, acc_s.shape[1]), f32)

        rows_loop(tokens, body)

    mine = pl.ds(pl.multiple_of(block * WIDE, WIDE), WIDE)
    for c in range(tokens // ROWS):
        r = pl.ds(c * ROWS, ROWS)
        aT_ref[:, r] = a_s[r, mine].T
        dyT_ref[:, r] = dy_ref[r, mine].T
        a = a_s[r, :]
        gate, up = nn(a, wg[0]), nn(a, wu[0])
        q, p = gates(gate, up)
        p_ref[r, :] = p
        q_ref[r, :] = q
        act = (q * up).astype(bf16)
        act_ref[r, :] = act
        acc_s[r, :] += nn(act, wd[0])

    @pl.when(block == n_blocks - 1)
    def _():
        def body(r):
            h_ref[r, :] = (x_ref[r, :].astype(f32) + acc_s[r, :].astype(bf16).astype(f32)).astype(bf16)

        rows_loop(tokens, body)


def forward(x, dy, wg, wu, wd):
    tokens, d = x.shape
    ff = wg.shape[2]
    n_blocks = ff // COLS
    whole = pl.BlockSpec((tokens, d), lambda b: (0, 0))
    wide = pl.BlockSpec((1, d, COLS), lambda b: (0, 0, b))
    hidden = pl.BlockSpec((tokens, COLS), lambda b: (0, b))
    turned = pl.BlockSpec((d // n_blocks, tokens), lambda b: (b, 0))
    return pl.pallas_call(
        functools.partial(forward_kernel, n_blocks),
        grid=(n_blocks,),
        out_shape=(
            jax.ShapeDtypeStruct((tokens, d), bf16),
            jax.ShapeDtypeStruct((tokens, ff), f32),
            jax.ShapeDtypeStruct((tokens, ff), f32),
            jax.ShapeDtypeStruct((tokens, ff), bf16),
            *(jax.ShapeDtypeStruct((d, tokens), bf16),) * 2,
        ),
        in_specs=[whole, whole, wide, wide, pl.BlockSpec((1, COLS, d), lambda b: (0, b, 0))],
        out_specs=(whole, hidden, hidden, hidden, turned, turned),
        scratch_shapes=[pltpu.VMEM((tokens, d), bf16), pltpu.VMEM((tokens, d), f32)],
        compiler_params=pltpu.CompilerParams(vmem_limit_bytes=VMEM_LIMIT),
        cost_estimate=pl.CostEstimate(flops=6 * tokens * d * ff, bytes_accessed=10 * tokens * ff, transcendentals=0),
        name="forward",
    )(x, dy, wg, wu, wd)


def dims_of(k):
    return k, (k + 1) % 3, (k + 2) % 3


def backward_kernel(n_blocks, count, aT_ref, dyT_ref, dy_ref, h_ref, p_ref, q_ref, act_ref, wg, wu, wd, *refs):
    outs, factor_ref = (refs[0:3], refs[3:6]), refs[6]
    (
        a_s, aT_s, dy_s, dyT_s, h_s, acc_s, wg_s, wu_s, wd_s, act_s, dg_s, du_s, p_s, q_s,
        own, f1, b2, f2, b3, ag, ssq, nrm,
        through1, through2, straight1, straight2, passed1, passed2, sums1, sums2, r3,
        w_sem, in_sem, pq_sem, act_sem, own_sem,
        snd1, snd2, rcv1, rcv2, s3_snd, s3_rcv, g1_snd, g1_rcv, g2_snd, g2_rcv, n_snd, n_rcv,
    ) = refs[7:]
    tokens, d = dy_s.shape
    steps = 2 * n_blocks
    me = lax.axis_index("dp")
    at = tuple(me // s % SIDE for s in STRIDE)
    offsets = (1, 3, 2)

    def to(dim, s):
        return {"dp": me + ((at[dim] + s) % SIDE - at[dim]) * STRIDE[dim]}

    def send(src, dst, snd, rcv, dim, s):
        return pltpu.make_async_remote_copy(src_ref=src, dst_ref=dst, send_sem=snd, recv_sem=rcv, device_id=to(dim, s), device_id_type=MESH)

    barrier = pltpu.get_barrier_semaphore()
    for dim in range(3):
        for s in offsets:
            pl.semaphore_signal(barrier, inc=1, device_id=to(dim, s), device_id_type=MESH)

    def columns(i):
        return pl.ds(pl.multiple_of(i * COLS, COLS), COLS)

    def load_up(i, slot):
        pairs = ((wg, wg_s), (wu, wu_s))
        return [pltpu.make_async_copy(w.at[1, :, columns(i)], to.at[slot], w_sem.at[slot, n]) for n, (w, to) in enumerate(pairs)]

    def load_down(layer, i, slot):
        return pltpu.make_async_copy(wd.at[layer, columns(i), :], wd_s.at[slot], w_sem.at[slot, 2])

    def load_pq(i):
        pairs = ((p_ref, p_s), (q_ref, q_s))
        return [pltpu.make_async_copy(src.at[:, columns(i)], to, pq_sem.at[n]) for n, (src, to) in enumerate(pairs)]

    def load_act(i):
        return pltpu.make_async_copy(act_ref.at[:, columns(i)], act_s, act_sem)

    def start(copies):
        for c in copies:
            c.start()

    def wait(copies):
        for c in copies:
            c.wait()

    load_h = pltpu.make_async_copy(h_ref, h_s, in_sem.at[0])
    load_dy = pltpu.make_async_copy(dy_ref, dy_s, in_sem.at[1])
    load_dyT = pltpu.make_async_copy(dyT_ref, dyT_s, in_sem.at[2])
    load_aT = pltpu.make_async_copy(aT_ref, aT_s, in_sem.at[2])
    start([load_h, load_dy, *load_up(0, 0), load_down(1, 0, 0), load_dyT, *load_pq(0)])
    ssq[...] = jnp.zeros_like(ssq)
    load_h.wait()

    def begin(r):
        a = normed(h_s[r, :])
        a_s[r, :] = a
        aT_s[:, r] = a.T
        acc_s[r, :] = jnp.zeros((r.size, d), f32)

    rows_loop(tokens, begin)
    wait([load_dy, load_dyT])
    pl.semaphore_wait(barrier, 9)

    def second_layer(i):
        slot = i % 2
        wait([*load_up(i, slot), load_down(1, i, slot)])

        @pl.when(i < n_blocks - 1)
        def _():
            start([*load_up(i + 1, 1 - slot), load_down(1, i + 1, 1 - slot)])

        @pl.when(i == n_blocks - 1)
        def _():
            load_down(0, 0, 1 - slot).start()

        for c in range(tokens // ROWS):
            r = pl.ds(c * ROWS, ROWS)
            a = a_s[r, :]
            gate, up = nn(a, wg_s[slot]), nn(a, wu_s[slot])
            by_act = nt(dy_s[r, :], wd_s[slot]).astype(bf16).astype(f32)
            q, p = gates(gate, up)
            act_s[r, :] = (q * up).astype(bf16)
            by_gate, by_up = (by_act * p).astype(bf16), (by_act * q).astype(bf16)
            dg_s[r, :] = by_gate
            du_s[r, :] = by_up
            acc_s[r, :] += nt(by_gate, wg_s[slot]) + nt(by_up, wu_s[slot])

    def between():
        load_aT.start()

        def back(r):
            wide = h_s[r, :].astype(f32)
            s = scale_of(wide)
            by_a = acc_s[r, :].astype(bf16).astype(f32)
            along = jnp.sum(by_a * wide, -1, keepdims=True)
            by_h = (by_a * s - wide * (s * s * s * along * (1.0 / d))).astype(bf16)
            total = (dy_s[r, :].astype(f32) + by_h.astype(f32)).astype(bf16)
            dy_s[r, :] = total
            dyT_s[:, r] = total.T

        rows_loop(tokens, back)
        load_aT.wait()

    def first_layer(i, block):
        slot = i % 2
        load_act(block).start()
        wait([load_down(0, block, slot), *load_pq(block)])

        @pl.when(block < n_blocks - 1)
        def _():
            load_down(0, block + 1, 1 - slot).start()

        for c in range(tokens // ROWS):
            r = pl.ds(c * ROWS, ROWS)
            by_act = nt(dy_s[r, :], wd_s[slot]).astype(bf16).astype(f32)
            dg_s[r, :] = (by_act * p_s[r, :]).astype(bf16)
            du_s[r, :] = (by_act * q_s[r, :]).astype(bf16)

        @pl.when(block < n_blocks - 1)
        def _():
            start(load_pq(block + 1))

        load_act(block).wait()

    def weight_gradient(slot, k):
        if k < 2:
            g = nn(aT_s[...], (dg_s, du_s)[k][...]).astype(bf16)
        else:
            g = nn(dyT_s[...], act_s[...]).astype(bf16)
        for p in range(SIDE):
            for q in range(SIDE):
                for r in range(SIDE):
                    row, col = ((p * SIDE + q), r) if k < 2 else ((q * SIDE + r), p)
                    own[slot, k, p, q, r] = g[row * HIGH : row * HIGH + HIGH, col * WIDE : col * WIDE + WIDE]

    stages = (
        (through1, straight1, passed1, sums1, snd1, rcv1),
        (through2, straight2, passed2, sums2, snd2, rcv2),
    )

    def piece(stage, j, k, whose, half):
        part = pl.ds(half * 2, 2)
        return b2.at[k, whose, part] if stage else own.at[j % own.shape[0], k, whose, part]

    def around(stage, k):
        c = at[dims_of(k)[stage]]
        return (c + 1) % SIDE, (c + 3) % SIDE, (c + 2) % SIDE

    def sends(stage, kind, j, k):
        buffers, snd, rcv = stages[stage][:3], stages[stage][-2], stages[stage][-1]
        nxt, prv, far = around(stage, k)
        slot = j % buffers[kind].shape[0]
        copies = []
        for half in range(2):
            down = half == 0 if kind != 1 else half == 1
            src = stages[stage][3].at[k, half] if kind == 2 else piece(stage, j, k, (nxt, prv)[half] if kind else far, half)
            copies.append(
                send(src, buffers[kind].at[slot, k, half], snd.at[kind, j % 2, k, half], rcv.at[kind, slot, k, half], dims_of(k)[stage], 3 if down else 1)
            )
        return copies

    def pass_on(stage, j):
        through, sums = stages[stage][0], stages[stage][3]
        slot, own_slot = j % 2, j % own.shape[0]
        for k in range(3):
            nxt, prv, _ = around(stage, k)
            onward = sends(stage, 2, j, k)
            for c in sends(stage, 0, j, k):
                c.wait_recv()
            for half, whose in enumerate((prv, nxt)):
                for q in range(2):
                    if stage:
                        sums[k, half, q] = (through[slot, k, half, q].astype(f32) + f1[k, whose, half * 2 + q]).astype(bf16)
                    else:
                        for r in range(SIDE):
                            mine = own[own_slot, k, whose, half * 2 + q, r].astype(f32)
                            sums[k, half, q, r] = (through[slot, k, half, q, r].astype(f32) + mine).astype(bf16)
                onward[half].start()
        if stage:
            done_sending(stage, (0, 1), j)

    def done_sending(stage, kinds, j):
        for k in range(3):
            for kind in kinds:
                for c in sends(stage, kind, j, k):
                    c.wait_send()

    def sum_1(j):
        slot, far_slot, own_slot = j % 2, j % straight1.shape[0], j % own.shape[0]
        for k in range(3):
            c = at[dims_of(k)[0]]
            for half in range(2):
                sends(0, 1, j, k)[half].wait_recv()
                sends(0, 2, j, k)[half].wait_recv()
                for q in range(2):
                    for r in range(SIDE):
                        total = own[own_slot, k, c, half * 2 + q, r].astype(f32) + passed1[slot, k, half, q, r].astype(f32)
                        total = total + straight1[far_slot, k, half, q, r].astype(f32)
                        f1[k, half * 2 + q, r] = total
                        b2[k, half * 2 + q, r] = total.astype(bf16)
            start(sends(1, 0, j, k) + sends(1, 1, j, k))
        done_sending(0, range(3), j)

    def sum_2(j):
        slot = j % 2
        for k in range(3):
            c = at[dims_of(k)[1]]
            for half in range(2):
                sends(1, 1, j, k)[half].wait_recv()
                sends(1, 2, j, k)[half].wait_recv()
                for q in range(2):
                    total = f1[k, c, half * 2 + q] + passed2[slot, k, half, q].astype(f32) + straight2[slot, k, half, q].astype(f32)
                    f2[k, half * 2 + q] = total
                    b3[k, half * 2 + q] = total.astype(bf16)
            start(sends_3(slot, k))
        done_sending(1, (2,), j)

    def sends_3(slot, k):
        r = dims_of(k)[2]
        return [send(b3.at[k, (at[r] + s) % SIDE], r3.at[slot, k, s - 1], s3_snd.at[k, s - 1], s3_rcv.at[slot, k, s - 1], r, s) for s in offsets]

    def sends_g1(j, k):
        r = dims_of(k)[2]
        mine = ag.at[j, k, at[r]]
        return [send(mine, mine, g1_snd.at[j, k, s - 1], g1_rcv.at[j, k, s - 1], r, s) for s in offsets]

    def sum_3(j):
        slot = j % 2
        for k in range(3):
            for c in sends_3(slot, k):
                c.wait_recv()
            total = f2[k, at[dims_of(k)[2]]]
            for s in range(3):
                total = total + r3[slot, k, s].astype(f32)
            g = total.astype(bf16)
            ag[j, k, at[dims_of(k)[2]]] = g
            start(sends_g1(j, k))
            wide = g.astype(f32)
            wide = wide * wide
            for row in range(0, HIGH, 8):
                ssq[...] += wide[row : row + 8]
        for k in range(3):
            for c in sends_3(slot, k):
                c.wait_send()

    def by_half(j, do):
        @pl.when(j < n_blocks)
        def _():
            do(j, outs[0])

        @pl.when(j >= n_blocks)
        def _():
            do(j - n_blocks, outs[1])

    def sends_g2(j, block, out, k):
        q = dims_of(k)[1]
        mine = ag.at[j, k]
        return [send(mine, out[k].at[block, at[q]], g2_snd.at[0, j, k, way], g2_rcv.at[0, j, k, way], q, s) for way, s in enumerate((1, 3))]

    def keep_g2(j, block, out, k):
        return pltpu.make_async_copy(ag.at[j, k], out[k].at[block, at[dims_of(k)[1]]], own_sem.at[j, k])

    def sends_g3(j, block, out, k):
        q = dims_of(k)[1]
        copies = []
        for way, s in enumerate((1, 3)):
            part = out[k].at[block, (at[q] + SIDE - s) % SIDE, pl.ds(way * 2, 2)]
            copies.append(send(part, part, g2_snd.at[1, j, k, way], g2_rcv.at[1, j, k, way], q, s))
        return copies

    def share(j):
        for k in range(3):
            wait(sends_g1(j, k))

        def do(block, out):
            for k in range(3):
                start(sends_g2(j, block, out, k) + [keep_g2(j, block, out, k)])

        by_half(j, do)

    def share_on(j):
        def do(block, out):
            for k in range(3):
                for there, on in zip(sends_g2(j, block, out, k), sends_g3(j, block, out, k), strict=True):
                    there.wait_recv()
                    on.start()

        by_half(j, do)

    def shared(j):
        def do(block, out):
            for k in range(3):
                for c in sends_g2(j, block, out, k):
                    c.wait_send()
                keep_g2(j, block, out, k).wait()
                wait(sends_g3(j, block, out, k))

        by_half(j, do)

    def sends_n(stage):
        mine = nrm.at[stage, at[stage]]
        return [send(mine, mine, n_snd.at[stage, s - 1], n_rcv.at[stage, s - 1], stage, s) for s in offsets]

    def norm_send(stage, value):
        nrm[stage, at[stage]] = value
        start(sends_n(stage))

    def norm_take(stage):
        wait(sends_n(stage))
        total = nrm[stage, 0]
        for s in range(1, SIDE):
            total = total + nrm[stage, s]
        return total

    def when(i, lag, do, *args):
        pl.when((i >= lag) & (i < steps + lag))(lambda: do(*args, i - lag))

    def each(do, low, high):
        def one(j, _):
            do(j)
            return 0

        lax.fori_loop(low, high, one, 0)

    def due(i):
        early = n_blocks // 2
        late = jnp.minimum(n_blocks + early * (i - steps), i - 3)
        return jnp.where(i < steps, jnp.clip(i - 3, 0, early), late)

    def step(i, _):
        @pl.when(i < n_blocks)
        def _():
            second_layer(i)

        @pl.when(i == n_blocks)
        def _():
            between()

        @pl.when((i >= n_blocks) & (i < steps))
        def _():
            first_layer(i, i - n_blocks)

        @pl.when(i < steps)
        def _():
            weight_gradient(i % own.shape[0], 0)

        when(i, 3, sum_2)
        when(i, 2, sum_1)
        when(i, 1, pass_on, 0)

        @pl.when(i == steps + 3)
        def _():
            norm_send(1, norm_take(0))

        each(share_on, due(i - 2), due(i - 1))
        each(share, due(i - 1), due(i))

        @pl.when(i < steps)
        def _():
            for k in range(3):
                if k:
                    weight_gradient(i % own.shape[0], k)
                start(sends(0, 0, i, k) + sends(0, 1, i, k))

        when(i, 2, pass_on, 1)
        when(i, 3, sum_3)

        @pl.when(i == steps + 2)
        def _():
            norm_send(0, ssq[...])

        return 0

    lax.fori_loop(0, steps + 4, step, 0)
    norm_send(2, norm_take(1))
    each(share_on, steps - 1, steps)
    total = jnp.sum(norm_take(2), keepdims=True)
    factor = jnp.minimum(1.0, 0.5 * lax.rsqrt(total * (1.0 / count) + 1e-30))
    factor_ref[...] = jnp.broadcast_to(factor, factor_ref.shape)
    each(shared, 0, steps)


def backward(aT, dyT, dy, h, p, q, act, wg, wu, wd):
    tokens, d = dy.shape
    ff = wg.shape[2]
    n_blocks = ff // COLS
    steps = 2 * n_blocks
    anywhere = pl.BlockSpec(memory_space=pl.ANY)
    shard = (HIGH, WIDE)
    quarter = jax.ShapeDtypeStruct((n_blocks, SIDE, SIDE, *shard), bf16)

    def dma(*shape):
        return pltpu.SemaphoreType.DMA(shape)

    def narrow(*shape):
        return pltpu.VMEM(shape, bf16)

    def wide(*shape):
        return pltpu.VMEM(shape, f32)

    halves1, halves2 = (3, 2, 2, SIDE, *shard), (3, 2, 2, *shard)
    return pl.pallas_call(
        functools.partial(backward_kernel, n_blocks, float(6 * d * ff)),
        out_shape=(quarter,) * 6 + (jax.ShapeDtypeStruct((8, 128), f32),),
        in_specs=[anywhere] * 10,
        out_specs=(anywhere,) * 6 + (pl.BlockSpec(memory_space=pltpu.VMEM),),
        scratch_shapes=[
            *(narrow(tokens, d), narrow(d, tokens)) * 2,
            narrow(tokens, d),
            wide(tokens, d),
            *(narrow(2, d, COLS),) * 2,
            narrow(2, COLS, d),
            *(narrow(tokens, COLS),) * 3,
            *(wide(tokens, COLS),) * 2,
            narrow(3, 3, SIDE, SIDE, SIDE, *shard),
            wide(3, SIDE, SIDE, *shard),
            narrow(3, SIDE, SIDE, *shard),
            wide(3, SIDE, *shard),
            narrow(3, SIDE, *shard),
            narrow(steps, 3, SIDE, *shard),
            wide(8, 128),
            wide(3, SIDE, 8, 128),
            narrow(2, *halves1),
            narrow(2, *halves2),
            narrow(3, *halves1),
            narrow(2, *halves2),
            narrow(2, *halves1),
            narrow(2, *halves2),
            narrow(*halves1),
            narrow(*halves2),
            narrow(2, 3, 3, *shard),
            dma(2, 3),
            dma(3),
            dma(2),
            dma(),
            dma(steps, 3),
            *(dma(3, 2, 3, 2),) * 2,
            *(dma(3, 3, 3, 2),) * 2,
            dma(3, 3),
            dma(2, 3, 3),
            *(dma(steps, 3, 3),) * 2,
            *(dma(2, steps, 3, 2),) * 2,
            *(dma(3, 3),) * 2,
        ],
        compiler_params=pltpu.CompilerParams(vmem_limit_bytes=VMEM_LIMIT, collective_id=0, has_side_effects=True),
        cost_estimate=pl.CostEstimate(flops=24 * tokens * d * ff, bytes_accessed=10 * tokens * ff, transcendentals=0),
        name="backward",
    )(aT, dyT, dy, h, p, q, act, wg, wu, wd)


def adamw_tile(factor, w, m, v, g):
    g = g.astype(f32) * factor
    m = 0.9 * m + 0.1 * g
    v = 0.95 * v + 0.05 * (g * g)
    wide = w.astype(f32)
    return (wide - 0.02 * (m * lax.rsqrt(v + 1e-8) + 0.1 * wide)).astype(bf16), m, v


def adamw_kernel(parts, shifts, n_blocks, factor_ref, *refs):
    n = len(parts)
    refs = list(refs)

    def take(count):
        taken = refs[:count]
        del refs[:count]
        return taken

    grads, arrays = take(3 * n), take(9)
    g_sem, in_sem, out_sem = refs[-3:]
    new, g_s, ins, outs = refs[-33:-24], refs[-24:-21], refs[-21:-12], refs[-12:-3]
    factor = factor_ref[...]
    me = lax.axis_index("dp")
    at = tuple(me // s % SIDE for s in STRIDE)
    steps = n * n_blocks

    def tile(k, i):
        part, block = i // n_blocks, i % n_blocks
        layer, shift = parts[0], shifts[0]
        if n > 1:
            layer, shift = layer + (parts[1] - layer) * part, shift + (shifts[1] - shift) * part
        quarter = (at[k] + shift + SIDE) % SIDE
        rows, cols = ins[k].shape[1:]
        if k < 2:
            return layer, pl.ds(pl.multiple_of(quarter * rows, rows), rows), pl.ds(pl.multiple_of(block * cols, cols), cols)
        row = pl.multiple_of((SIDE * block + quarter) * rows, rows)
        return layer, pl.ds(row, rows), slice(None)

    def loads(k, i):
        slot = i % AHEAD
        return [
            pltpu.make_async_copy(arrays[j].at[tile(k, i)], ins[j].at[slot], in_sem.at[slot, j]) for j in range(k, 9, 3)
        ]

    def load_g(k, i, part):
        slot = i % AHEAD
        return pltpu.make_async_copy(grads[3 * part + k].at[i % n_blocks], g_s[k].at[slot], g_sem.at[slot, k])

    def start(k, i):
        for c in loads(k, i):
            c.start()
        for part in range(n):

            @pl.when(i // n_blocks == part)
            def _():
                load_g(k, i, part).start()

    def stores(k, i):
        slot = i % 2
        return [
            pltpu.make_async_copy(outs[j].at[slot], new[j].at[tile(k, i)], out_sem.at[slot, j]) for j in range(k, 9, 3)
        ]

    def wait(k, i):
        for c in stores(k, i):
            c.wait()

    def first(i, _):
        for k in range(3):
            start(k, i)
        return 0

    lax.fori_loop(0, AHEAD, first, 0)

    def step(i, _):
        slot, out = i % AHEAD, i % 2
        for k in range(3):
            for c in loads(k, i):
                c.wait()
            load_g(k, i, 0).wait()

            @pl.when(i >= 2)
            def _():
                wait(k, i - 2)

            def one(where, g):
                done = adamw_tile(factor[0:1, 0:1], *(ins[j][(slot, *where)] for j in range(k, 9, 3)), g)
                for j, value in zip(range(k, 9, 3), done, strict=True):
                    outs[j][(out, *where)] = value

            if k < 2:
                for q in range(SIDE):
                    for r in range(SIDE):
                        one((pl.ds(q * HIGH, HIGH), pl.ds(r * WIDE, WIDE)), g_s[k][slot, q, r])
            else:
                for lo in range(0, SIDE * SIDE * HIGH, WIDE):
                    pieces = [divmod(e, HIGH) for e in range(lo, lo + WIDE, 16)]
                    rows = [g_s[k][slot, n // SIDE, n % SIDE, pl.ds(row, 16)] for n, row in pieces]
                    one((slice(None), pl.ds(lo, WIDE)), jnp.concatenate(rows, 0).T)
            for c in stores(k, i):
                c.start()

            @pl.when(i + AHEAD < steps)
            def _():
                start(k, i + AHEAD)

        return 0

    lax.fori_loop(0, steps, step, 0)
    for k in range(3):
        wait(k, steps - 2)
        wait(k, steps - 1)


def adamw(parts, shifts, factor, grads, w, m, v, into):
    n, n_blocks = len(parts), grads[0].shape[0]
    d, ff = w[0].shape[1:]
    arrays = list(w) + list(m) + list(v)
    anywhere = pl.BlockSpec(memory_space=pl.ANY)
    tiles = [(d // SIDE, COLS), (d // SIDE, COLS), (COLS // SIDE, d)] * 3
    old = list(into or [])
    return pl.pallas_call(
        functools.partial(adamw_kernel, parts, shifts, n_blocks),
        out_shape=tuple(jax.ShapeDtypeStruct(a.shape, a.dtype) for a in arrays),
        in_specs=[pl.BlockSpec(memory_space=pltpu.VMEM)] + [anywhere] * (len(grads) + 9 + len(old)),
        out_specs=(anywhere,) * 9,
        input_output_aliases={1 + len(grads) + 9 + j: j for j in range(len(old))},
        scratch_shapes=[pltpu.VMEM((AHEAD, *grads[0].shape[1:]), bf16)] * 3
        + [pltpu.VMEM((AHEAD, *t), a.dtype) for t, a in zip(tiles, arrays, strict=True)]
        + [pltpu.VMEM((2, *t), a.dtype) for t, a in zip(tiles, arrays, strict=True)]
        + [pltpu.SemaphoreType.DMA(s) for s in ((AHEAD, 3), (AHEAD, 9), (2, 9))],
        compiler_params=pltpu.CompilerParams(vmem_limit_bytes=VMEM_LIMIT),
        cost_estimate=pl.CostEstimate(flops=n * 45_000_000_000, bytes_accessed=n * 16 * d * ff, transcendentals=0),
        name="adamw",
    )(factor, *grads, *arrays, *old)


def ring(dim, s):
    pairs = []
    for i in range(SIDE**3):
        c = i // STRIDE[dim] % SIDE
        pairs.append((i, i + ((c + s) % SIDE - c) * STRIDE[dim]))
    return pairs


def solution(mesh):
    def step(x, dy, *arrays):
        w, m, v = (arrays[i : i + 3] for i in (0, 3, 6))
        x, dy = x[0], dy[0]
        h, p, q, act, aT, dyT = forward(x, dy, *w)
        *quarters, factor = backward(aT, dyT, dy, h, p, q, act, *w)
        second, first = quarters[0:3], quarters[3:6]

        def shift(parts, s):
            return [lax.ppermute(g, "dp", ring(k, s)) for k, g in enumerate(parts)]

        second_up, second_down = shift(second, 1), shift(second, -1)
        first_up, first_down = shift(first, 1), shift(first, -1)
        new = adamw([1, 0], [0, 0], factor, second + first, w, m, v, None)
        second_up, second_down, new = lax.optimization_barrier((second_up, second_down, new))
        second_far = shift(second_up, 1)
        new = adamw([1, 1], [-1, 1], factor, second_up + second_down, w, m, v, new)
        first_up, first_down, new = lax.optimization_barrier((first_up, first_down, new))
        first_far = shift(first_down, -1)
        new = adamw([0, 0], [-1, 1], factor, first_up + first_down, w, m, v, new)
        second_far, first_far, new = lax.optimization_barrier((second_far, first_far, new))
        new = adamw([1, 0], [2, 2], factor, second_far + first_far, w, m, v, new)
        return tuple(new)

    return jax.shard_map(
        step,
        mesh=mesh,
        in_specs=(P(("rep", "dp"), None, None),) * 2 + (P(None, None, None),) * 9,
        out_specs=(P("rep", None, None),) * 9,
        check_vma=False,
    )
```

```python
import functools

import jax
import jax.numpy as jnp
from jax import lax
from jax.experimental import pallas as pl
from jax.experimental.pallas import tpu as pltpu
from jax.sharding import PartitionSpec as P

f32, bf16 = jnp.float32, jnp.bfloat16
MESH = pl.DeviceIdType.MESH
SIDE = 4
STRIDE = (16, 4, 1)
COLS = 512
ROWS = 512
HIGH, WIDE = 48, 128
AHEAD = 4
VMEM_LIMIT = 66_900_000


def nn(a, b):
    return jnp.dot(a, b, preferred_element_type=f32)


def nt(a, b):
    return lax.dot_general(a, b, (((1,), (1,)), ((), ())), preferred_element_type=f32)


def scale_of(wide):
    return lax.rsqrt(jnp.mean(wide * wide, -1, keepdims=True) + 1e-6)


def normed(h):
    wide = h.astype(f32)
    return (wide * scale_of(wide)).astype(bf16)


def gates(gate, up):
    sig = 1.0 / (1.0 + jnp.exp(-gate))
    q = gate * sig
    return q, up * (sig + q * (1.0 - sig))


def rows_loop(tokens, body, step=256):
    def one(c, _):
        body(pl.ds(pl.multiple_of(c * step, step), step))
        return 0

    lax.fori_loop(0, tokens // step, one, 0)


def forward_kernel(n_blocks, x_ref, dy_ref, wg, wu, wd, h_ref, p_ref, q_ref, act_ref, aT_ref, dyT_ref, a_s, acc_s):
    block = pl.program_id(0)
    tokens = x_ref.shape[0]

    @pl.when(block == 0)
    def _():
        def body(r):
            a_s[r, :] = normed(x_ref[r, :])
            acc_s[r, :] = jnp.zeros((256, acc_s.shape[1]), f32)

        rows_loop(tokens, body)

    part = dyT_ref.shape[0]
    mine = pl.ds(pl.multiple_of(block * part, part), part)
    for c in range(tokens // ROWS):
        r = pl.ds(c * ROWS, ROWS)
        aT_ref[:, r] = a_s[r, mine].T
        dyT_ref[:, r] = dy_ref[r, :].T
        a = a_s[r, :]
        gate, up = nn(a, wg[0]), nn(a, wu[0])
        q, p = gates(gate, up)
        p_ref[r, :] = p
        q_ref[r, :] = q
        act = (q * up).astype(bf16)
        act_ref[r, :] = act
        acc_s[r, :] += nn(act, wd[0])

    @pl.when(block == n_blocks - 1)
    def _():
        def body(r):
            h_ref[r, :] = (x_ref[r, :].astype(f32) + acc_s[r, :].astype(bf16).astype(f32)).astype(bf16)

        rows_loop(tokens, body)


def forward(x, dy, wg, wu, wd):
    tokens, d = x.shape
    ff = wg.shape[2]
    n_blocks = ff // COLS
    whole = pl.BlockSpec((tokens, d), lambda b: (0, 0))
    wide = pl.BlockSpec((1, d, COLS), lambda b: (0, 0, b))
    hidden = pl.BlockSpec((tokens, COLS), lambda b: (0, b))
    turned = pl.BlockSpec((d // n_blocks, tokens), lambda b: (b, 0))
    return pl.pallas_call(
        functools.partial(forward_kernel, n_blocks),
        grid=(n_blocks,),
        out_shape=(
            jax.ShapeDtypeStruct((tokens, d), bf16),
            jax.ShapeDtypeStruct((tokens, ff), f32),
            jax.ShapeDtypeStruct((tokens, ff), f32),
            jax.ShapeDtypeStruct((tokens, ff), bf16),
            *(jax.ShapeDtypeStruct((d, tokens), bf16),) * 2,
        ),
        in_specs=[whole, pl.BlockSpec((tokens, d // n_blocks), lambda b: (0, b)), wide, wide, pl.BlockSpec((1, COLS, d), lambda b: (0, b, 0))],
        out_specs=(whole, hidden, hidden, hidden, turned, turned),
        scratch_shapes=[pltpu.VMEM((tokens, d), bf16), pltpu.VMEM((tokens, d), f32)],
        compiler_params=pltpu.CompilerParams(vmem_limit_bytes=VMEM_LIMIT),
        cost_estimate=pl.CostEstimate(flops=6 * tokens * d * ff, bytes_accessed=10 * tokens * ff, transcendentals=0),
        name="forward",
    )(x, dy, wg, wu, wd)


def dims_of(k):
    return k, (k + 1) % 3, (k + 2) % 3


def backward_kernel(n_blocks, count, aT_ref, dyT_ref, dy_ref, h_ref, p_ref, q_ref, act_ref, wg, wu, wd, *refs):
    outs, factor_ref = (refs[0:3], refs[3:6]), refs[6]
    (
        a_s, aT_s, dy_s, dyT_s, h_s, acc_s, wg_s, wu_s, wd_s, act_s, dg_s, du_s, p_s, q_s,
        own, f1, b2, f2, b3, ag, ssq, nrm,
        through1, through2, straight1, straight2, passed1, passed2, sums1, sums2, r3,
        w_sem, in_sem, pq_sem, act_sem, own_sem,
        snd1, snd2, rcv1, rcv2, s3_snd, s3_rcv, g1_snd, g1_rcv, g2_snd, g2_rcv, n_snd, n_rcv,
    ) = refs[7:]
    tokens, d = dy_s.shape
    steps = 2 * n_blocks
    me = lax.axis_index("dp")
    at = tuple(me // s % SIDE for s in STRIDE)
    offsets = (1, 3, 2)

    def to(dim, s):
        return {"dp": me + ((at[dim] + s) % SIDE - at[dim]) * STRIDE[dim]}

    def send(src, dst, snd, rcv, dim, s):
        return pltpu.make_async_remote_copy(src_ref=src, dst_ref=dst, send_sem=snd, recv_sem=rcv, device_id=to(dim, s), device_id_type=MESH)

    barrier = pltpu.get_barrier_semaphore()
    for dim in range(3):
        for s in offsets:
            pl.semaphore_signal(barrier, inc=1, device_id=to(dim, s), device_id_type=MESH)

    def columns(i):
        return pl.ds(pl.multiple_of(i * COLS, COLS), COLS)

    def load_up(i, slot):
        pairs = ((wg, wg_s), (wu, wu_s))
        return [pltpu.make_async_copy(w.at[1, :, columns(i)], to.at[slot], w_sem.at[slot, n]) for n, (w, to) in enumerate(pairs)]

    def load_down(layer, i, slot):
        return pltpu.make_async_copy(wd.at[layer, columns(i), :], wd_s.at[slot], w_sem.at[slot, 2])

    def load_pq(i):
        pairs = ((p_ref, p_s), (q_ref, q_s))
        return [pltpu.make_async_copy(src.at[:, columns(i)], to, pq_sem.at[n]) for n, (src, to) in enumerate(pairs)]

    def load_act(i):
        return pltpu.make_async_copy(act_ref.at[:, columns(i)], act_s, act_sem)

    def start(copies):
        for c in copies:
            c.start()

    def wait(copies):
        for c in copies:
            c.wait()

    load_h = pltpu.make_async_copy(h_ref, h_s, in_sem.at[0])
    load_dy = pltpu.make_async_copy(dy_ref, dy_s, in_sem.at[1])
    load_dyT = pltpu.make_async_copy(dyT_ref, dyT_s, in_sem.at[2])
    load_aT = pltpu.make_async_copy(aT_ref, aT_s, in_sem.at[2])
    start([load_h, load_dy, *load_up(0, 0), load_down(1, 0, 0), load_dyT, *load_pq(0)])
    ssq[...] = jnp.zeros_like(ssq)
    load_h.wait()

    def begin(r):
        a = normed(h_s[r, :])
        a_s[r, :] = a
        aT_s[:, r] = a.T
        acc_s[r, :] = jnp.zeros((r.size, d), f32)

    rows_loop(tokens, begin)
    wait([load_dy, load_dyT])
    pl.semaphore_wait(barrier, 9)

    def second_layer(i):
        slot = i % 2
        wait([*load_up(i, slot), load_down(1, i, slot)])

        @pl.when(i < n_blocks - 1)
        def _():
            start([*load_up(i + 1, 1 - slot), load_down(1, i + 1, 1 - slot)])

        @pl.when(i == n_blocks - 1)
        def _():
            load_down(0, 0, 1 - slot).start()

        for c in range(tokens // ROWS):
            r = pl.ds(c * ROWS, ROWS)
            a = a_s[r, :]
            gate, up = nn(a, wg_s[slot]), nn(a, wu_s[slot])
            by_act = nt(dy_s[r, :], wd_s[slot]).astype(bf16).astype(f32)
            q, p = gates(gate, up)
            act_s[r, :] = (q * up).astype(bf16)
            by_gate, by_up = (by_act * p).astype(bf16), (by_act * q).astype(bf16)
            dg_s[r, :] = by_gate
            du_s[r, :] = by_up
            acc_s[r, :] += nt(by_gate, wg_s[slot]) + nt(by_up, wu_s[slot])

    def between():
        load_aT.start()

        def back(r):
            wide = h_s[r, :].astype(f32)
            s = scale_of(wide)
            by_a = acc_s[r, :].astype(bf16).astype(f32)
            along = jnp.sum(by_a * wide, -1, keepdims=True)
            by_h = (by_a * s - wide * (s * s * s * along * (1.0 / d))).astype(bf16)
            total = (dy_s[r, :].astype(f32) + by_h.astype(f32)).astype(bf16)
            dy_s[r, :] = total
            dyT_s[:, r] = total.T

        rows_loop(tokens, back)
        load_aT.wait()

    def first_layer(i, block):
        slot = i % 2
        load_act(block).start()
        wait([load_down(0, block, slot), *load_pq(block)])

        @pl.when(block < n_blocks - 1)
        def _():
            load_down(0, block + 1, 1 - slot).start()

        for c in range(tokens // ROWS):
            r = pl.ds(c * ROWS, ROWS)
            by_act = nt(dy_s[r, :], wd_s[slot]).astype(bf16).astype(f32)
            dg_s[r, :] = (by_act * p_s[r, :]).astype(bf16)
            du_s[r, :] = (by_act * q_s[r, :]).astype(bf16)

        @pl.when(block < n_blocks - 1)
        def _():
            start(load_pq(block + 1))

        load_act(block).wait()

    def weight_gradient(slot, k):
        if k < 2:
            g = nn(aT_s[...], (dg_s, du_s)[k][...]).astype(bf16)
        else:
            g = nn(dyT_s[...], act_s[...]).astype(bf16)
        for p in range(SIDE):
            for q in range(SIDE):
                for r in range(SIDE):
                    row, col = ((p * SIDE + q), r) if k < 2 else ((q * SIDE + r), p)
                    own[slot, k, p, q, r] = g[row * HIGH : row * HIGH + HIGH, col * WIDE : col * WIDE + WIDE]

    stages = (
        (through1, straight1, passed1, sums1, snd1, rcv1),
        (through2, straight2, passed2, sums2, snd2, rcv2),
    )

    def piece(stage, j, k, whose, half):
        part = pl.ds(half * 2, 2)
        return b2.at[k, whose, part] if stage else own.at[j % own.shape[0], k, whose, part]

    def around(stage, k):
        c = at[dims_of(k)[stage]]
        return (c + 1) % SIDE, (c + 3) % SIDE, (c + 2) % SIDE

    def sends(stage, kind, j, k):
        buffers, snd, rcv = stages[stage][:3], stages[stage][-2], stages[stage][-1]
        nxt, prv, far = around(stage, k)
        slot = j % buffers[kind].shape[0]
        copies = []
        for half in range(2):
            down = half == 0 if kind != 1 else half == 1
            src = stages[stage][3].at[k, half] if kind == 2 else piece(stage, j, k, (nxt, prv)[half] if kind else far, half)
            copies.append(
                send(src, buffers[kind].at[slot, k, half], snd.at[kind, j % 2, k, half], rcv.at[kind, slot, k, half], dims_of(k)[stage], 3 if down else 1)
            )
        return copies

    def pass_on(stage, j):
        through, sums = stages[stage][0], stages[stage][3]
        slot, own_slot = j % 2, j % own.shape[0]
        for k in range(3):
            nxt, prv, _ = around(stage, k)
            onward = sends(stage, 2, j, k)
            for c in sends(stage, 0, j, k):
                c.wait_recv()
            for half, whose in enumerate((prv, nxt)):
                for q in range(2):
                    if stage:
                        sums[k, half, q] = (through[slot, k, half, q].astype(f32) + f1[slot, k, whose, half * 2 + q]).astype(bf16)
                    else:
                        for r in range(SIDE):
                            mine = own[own_slot, k, whose, half * 2 + q, r].astype(f32)
                            sums[k, half, q, r] = (through[slot, k, half, q, r].astype(f32) + mine).astype(bf16)
                onward[half].start()
        if stage:
            done_sending(stage, (0, 1), j)

    def done_sending(stage, kinds, j):
        for k in range(3):
            for kind in kinds:
                for c in sends(stage, kind, j, k):
                    c.wait_send()

    def sum_1(j):
        slot, far_slot, own_slot = j % 2, j % straight1.shape[0], j % own.shape[0]
        for k in range(3):
            c = at[dims_of(k)[0]]
            for half in range(2):
                sends(0, 1, j, k)[half].wait_recv()
                sends(0, 2, j, k)[half].wait_recv()
                for q in range(2):
                    for r in range(SIDE):
                        total = own[own_slot, k, c, half * 2 + q, r].astype(f32) + passed1[slot, k, half, q, r].astype(f32)
                        total = total + straight1[far_slot, k, half, q, r].astype(f32)
                        f1[slot, k, half * 2 + q, r] = total
                        b2[k, half * 2 + q, r] = total.astype(bf16)
            start(sends(1, 0, j, k) + sends(1, 1, j, k))
        done_sending(0, range(3), j)

    def sum_2(j):
        slot, far_slot = j % 2, j % straight2.shape[0]
        for k in range(3):
            c = at[dims_of(k)[1]]
            for half in range(2):
                sends(1, 1, j, k)[half].wait_recv()
                sends(1, 2, j, k)[half].wait_recv()
                for q in range(2):
                    total = f1[slot, k, c, half * 2 + q] + passed2[slot, k, half, q].astype(f32)
                    total = total + straight2[far_slot, k, half, q].astype(f32)
                    f2[k, half * 2 + q] = total
                    b3[k, half * 2 + q] = total.astype(bf16)
            start(sends_3(slot, k))
        done_sending(1, (2,), j)

    def sends_3(slot, k):
        r = dims_of(k)[2]
        return [send(b3.at[k, (at[r] + s) % SIDE], r3.at[slot, k, s - 1], s3_snd.at[k, s - 1], s3_rcv.at[slot, k, s - 1], r, s) for s in offsets]

    def sends_g1(j, k):
        r = dims_of(k)[2]
        mine = ag.at[j, k, at[r]]
        return [send(mine, mine, g1_snd.at[j, k, s - 1], g1_rcv.at[j, k, s - 1], r, s) for s in offsets]

    def sum_3(j):
        slot = j % 2
        for k in range(3):
            for c in sends_3(slot, k):
                c.wait_recv()
            total = f2[k, at[dims_of(k)[2]]]
            for s in range(3):
                total = total + r3[slot, k, s].astype(f32)
            g = total.astype(bf16)
            ag[j, k, at[dims_of(k)[2]]] = g
            start(sends_g1(j, k))
            wide = g.astype(f32)
            wide = wide * wide
            for row in range(0, HIGH, 8):
                ssq[...] += wide[row : row + 8]
        for k in range(3):
            for c in sends_3(slot, k):
                c.wait_send()

    def by_half(j, do):
        @pl.when(j < n_blocks)
        def _():
            do(j, outs[0])

        @pl.when(j >= n_blocks)
        def _():
            do(j - n_blocks, outs[1])

    def sends_g2(j, block, out, k):
        q = dims_of(k)[1]
        mine = ag.at[j, k]
        return [send(mine, out[k].at[block, at[q]], g2_snd.at[0, j, k, way], g2_rcv.at[0, j, k, way], q, s) for way, s in enumerate((1, 3))]

    def keep_g2(j, block, out, k):
        return pltpu.make_async_copy(ag.at[j, k], out[k].at[block, at[dims_of(k)[1]]], own_sem.at[j, k])

    def sends_g3(j, block, out, k):
        q = dims_of(k)[1]
        copies = []
        for way, s in enumerate((1, 3)):
            part = out[k].at[block, (at[q] + SIDE - s) % SIDE, pl.ds(way * 2, 2)]
            copies.append(send(part, part, g2_snd.at[1, j, k, way], g2_rcv.at[1, j, k, way], q, s))
        return copies

    def share(j):
        for k in range(3):
            wait(sends_g1(j, k))

        def do(block, out):
            for k in range(3):
                start(sends_g2(j, block, out, k) + [keep_g2(j, block, out, k)])

        by_half(j, do)

    def share_on(j):
        def do(block, out):
            for k in range(3):
                for there, on in zip(sends_g2(j, block, out, k), sends_g3(j, block, out, k), strict=True):
                    there.wait_recv()
                    on.start()

        by_half(j, do)

    def shared(j):
        def do(block, out):
            for k in range(3):
                for c in sends_g2(j, block, out, k):
                    c.wait_send()
                keep_g2(j, block, out, k).wait()
                wait(sends_g3(j, block, out, k))

        by_half(j, do)

    def sends_n(stage):
        mine = nrm.at[stage, at[stage]]
        return [send(mine, mine, n_snd.at[stage, s - 1], n_rcv.at[stage, s - 1], stage, s) for s in offsets]

    def norm_send(stage, value):
        nrm[stage, at[stage]] = value
        start(sends_n(stage))

    def norm_take(stage):
        wait(sends_n(stage))
        total = nrm[stage, 0]
        for s in range(1, SIDE):
            total = total + nrm[stage, s]
        return total

    def when(i, lag, do, *args):
        pl.when((i >= lag) & (i < steps + lag))(lambda: do(*args, i - lag))

    def each(do, low, high):
        def one(j, _):
            do(j)
            return 0

        lax.fori_loop(low, high, one, 0)

    def due(i):
        late = jnp.minimum(1 + 2 * (i + 1 - steps), i - 4)
        return jnp.where(i < steps, jnp.clip(i - 4, 0, 1), late)

    def step(i, _):
        @pl.when(i < n_blocks)
        def _():
            second_layer(i)

        @pl.when(i == n_blocks)
        def _():
            between()

        @pl.when((i >= n_blocks) & (i < steps))
        def _():
            first_layer(i, i - n_blocks)

        @pl.when(i < steps)
        def _():
            weight_gradient(i % own.shape[0], 0)

        when(i, 2, sum_1)
        when(i, 1, pass_on, 0)
        each(share_on, due(i - 2), due(i - 1))
        each(share, due(i - 1), due(i))

        @pl.when(i < steps)
        def _():
            for k in range(3):
                if k:
                    weight_gradient(i % own.shape[0], k)
                start(sends(0, 0, i, k) + sends(0, 1, i, k))

        when(i, 4, sum_3)

        @pl.when(i == steps + 3)
        def _():
            norm_send(0, ssq[...])

        when(i, 3, sum_2)
        when(i, 2, pass_on, 1)
        return 0

    lax.fori_loop(0, steps + 4, step, 0)
    norm_send(1, norm_take(0))
    begun = 1 + 2 * SIDE
    each(share_on, begun - 2, begun)
    each(share, begun, steps)
    norm_send(2, norm_take(1))
    each(share_on, begun, steps)
    total = jnp.sum(norm_take(2), keepdims=True)
    factor = jnp.minimum(1.0, 0.5 * lax.rsqrt(total * (1.0 / count) + 1e-30))
    factor_ref[...] = jnp.broadcast_to(factor, factor_ref.shape)
    each(shared, 0, steps)


def backward(aT, dyT, dy, h, p, q, act, wg, wu, wd):
    tokens, d = dy.shape
    ff = wg.shape[2]
    n_blocks = ff // COLS
    steps = 2 * n_blocks
    anywhere = pl.BlockSpec(memory_space=pl.ANY)
    shard = (HIGH, WIDE)
    quarter = jax.ShapeDtypeStruct((n_blocks, SIDE, SIDE, *shard), bf16)

    def dma(*shape):
        return pltpu.SemaphoreType.DMA(shape)

    def narrow(*shape):
        return pltpu.VMEM(shape, bf16)

    def wide(*shape):
        return pltpu.VMEM(shape, f32)

    halves1, halves2 = (3, 2, 2, SIDE, *shard), (3, 2, 2, *shard)
    return pl.pallas_call(
        functools.partial(backward_kernel, n_blocks, float(6 * d * ff)),
        out_shape=(quarter,) * 6 + (jax.ShapeDtypeStruct((8, 128), f32),),
        in_specs=[anywhere] * 10,
        out_specs=(anywhere,) * 6 + (pl.BlockSpec(memory_space=pltpu.VMEM),),
        scratch_shapes=[
            *(narrow(tokens, d), narrow(d, tokens)) * 2,
            narrow(tokens, d),
            wide(tokens, d),
            *(narrow(2, d, COLS),) * 2,
            narrow(2, COLS, d),
            *(narrow(tokens, COLS),) * 3,
            *(wide(tokens, COLS),) * 2,
            narrow(3, 3, SIDE, SIDE, SIDE, *shard),
            wide(2, 3, SIDE, SIDE, *shard),
            narrow(3, SIDE, SIDE, *shard),
            wide(3, SIDE, *shard),
            narrow(3, SIDE, *shard),
            narrow(steps, 3, SIDE, *shard),
            wide(8, 128),
            wide(3, SIDE, 8, 128),
            narrow(2, *halves1),
            narrow(2, *halves2),
            narrow(3, *halves1),
            narrow(3, *halves2),
            narrow(2, *halves1),
            narrow(2, *halves2),
            narrow(*halves1),
            narrow(*halves2),
            narrow(2, 3, 3, *shard),
            dma(2, 3),
            dma(3),
            dma(2),
            dma(),
            dma(steps, 3),
            *(dma(3, 2, 3, 2),) * 2,
            *(dma(3, 3, 3, 2),) * 2,
            dma(3, 3),
            dma(2, 3, 3),
            *(dma(steps, 3, 3),) * 2,
            *(dma(2, steps, 3, 2),) * 2,
            *(dma(3, 3),) * 2,
        ],
        compiler_params=pltpu.CompilerParams(vmem_limit_bytes=VMEM_LIMIT, collective_id=0, has_side_effects=True),
        cost_estimate=pl.CostEstimate(flops=24 * tokens * d * ff, bytes_accessed=10 * tokens * ff, transcendentals=0),
        name="backward",
    )(aT, dyT, dy, h, p, q, act, wg, wu, wd)


def adamw_tile(factor, w, m, v, g):
    g = g.astype(f32) * factor
    m = 0.9 * m + 0.1 * g
    v = 0.95 * v + 0.05 * (g * g)
    wide = w.astype(f32)
    return (wide - 0.02 * (m * lax.rsqrt(v + 1e-8) + 0.1 * wide)).astype(bf16), m, v


def adamw_kernel(parts, shifts, n_blocks, factor_ref, *refs):
    n = len(parts)
    refs = list(refs)

    def take(count):
        taken = refs[:count]
        del refs[:count]
        return taken

    grads, arrays = take(3 * n), take(9)
    g_sem, in_sem, out_sem = refs[-3:]
    new, g_s, ins, outs = refs[-33:-24], refs[-24:-21], refs[-21:-12], refs[-12:-3]
    factor = factor_ref[...]
    me = lax.axis_index("dp")
    at = tuple(me // s % SIDE for s in STRIDE)
    steps = n * n_blocks

    def tile(k, i):
        part, block = i // n_blocks, i % n_blocks
        layer, shift = parts[0], shifts[0]
        if n > 1:
            layer, shift = layer + (parts[1] - layer) * part, shift + (shifts[1] - shift) * part
        quarter = (at[k] + shift + SIDE) % SIDE
        rows, cols = ins[k].shape[1:]
        if k < 2:
            return layer, pl.ds(pl.multiple_of(quarter * rows, rows), rows), pl.ds(pl.multiple_of(block * cols, cols), cols)
        row = pl.multiple_of((SIDE * block + quarter) * rows, rows)
        return layer, pl.ds(row, rows), slice(None)

    def loads(k, i):
        slot = i % AHEAD
        return [
            pltpu.make_async_copy(arrays[j].at[tile(k, i)], ins[j].at[slot], in_sem.at[slot, j]) for j in range(k, 9, 3)
        ]

    def load_g(k, i, part):
        slot = i % AHEAD
        return pltpu.make_async_copy(grads[3 * part + k].at[i % n_blocks], g_s[k].at[slot], g_sem.at[slot, k])

    def start(k, i):
        for c in loads(k, i):
            c.start()
        for part in range(n):

            @pl.when(i // n_blocks == part)
            def _():
                load_g(k, i, part).start()

    def stores(k, i):
        slot = i % 2
        return [
            pltpu.make_async_copy(outs[j].at[slot], new[j].at[tile(k, i)], out_sem.at[slot, j]) for j in range(k, 9, 3)
        ]

    def wait(k, i):
        for c in stores(k, i):
            c.wait()

    def first(i, _):
        for k in range(3):
            start(k, i)
        return 0

    lax.fori_loop(0, AHEAD, first, 0)

    def step(i, _):
        slot, out = i % AHEAD, i % 2
        for k in range(3):
            for c in loads(k, i):
                c.wait()
            load_g(k, i, 0).wait()

            @pl.when(i >= 2)
            def _():
                wait(k, i - 2)

            def one(where, g):
                done = adamw_tile(factor[0:1, 0:1], *(ins[j][(slot, *where)] for j in range(k, 9, 3)), g)
                for j, value in zip(range(k, 9, 3), done, strict=True):
                    outs[j][(out, *where)] = value

            if k < 2:
                for q in range(SIDE):
                    for r in range(SIDE):
                        one((pl.ds(q * HIGH, HIGH), pl.ds(r * WIDE, WIDE)), g_s[k][slot, q, r])
            else:
                for lo in range(0, SIDE * SIDE * HIGH, WIDE):
                    pieces = [divmod(e, HIGH) for e in range(lo, lo + WIDE, 16)]
                    rows = [g_s[k][slot, n // SIDE, n % SIDE, pl.ds(row, 16)] for n, row in pieces]
                    one((slice(None), pl.ds(lo, WIDE)), jnp.concatenate(rows, 0).T)
            for c in stores(k, i):
                c.start()

            @pl.when(i + AHEAD < steps)
            def _():
                start(k, i + AHEAD)

        return 0

    lax.fori_loop(0, steps, step, 0)
    for k in range(3):
        wait(k, steps - 2)
        wait(k, steps - 1)


def adamw(parts, shifts, factor, grads, w, m, v, into):
    n, n_blocks = len(parts), grads[0].shape[0]
    d, ff = w[0].shape[1:]
    arrays = list(w) + list(m) + list(v)
    anywhere = pl.BlockSpec(memory_space=pl.ANY)
    tiles = [(d // SIDE, COLS), (d // SIDE, COLS), (COLS // SIDE, d)] * 3
    old = list(into or [])
    return pl.pallas_call(
        functools.partial(adamw_kernel, parts, shifts, n_blocks),
        out_shape=tuple(jax.ShapeDtypeStruct(a.shape, a.dtype) for a in arrays),
        in_specs=[pl.BlockSpec(memory_space=pltpu.VMEM)] + [anywhere] * (len(grads) + 9 + len(old)),
        out_specs=(anywhere,) * 9,
        input_output_aliases={1 + len(grads) + 9 + j: j for j in range(len(old))},
        scratch_shapes=[pltpu.VMEM((AHEAD, *grads[0].shape[1:]), bf16)] * 3
        + [pltpu.VMEM((AHEAD, *t), a.dtype) for t, a in zip(tiles, arrays, strict=True)]
        + [pltpu.VMEM((2, *t), a.dtype) for t, a in zip(tiles, arrays, strict=True)]
        + [pltpu.SemaphoreType.DMA(s) for s in ((AHEAD, 3), (AHEAD, 9), (2, 9))],
        compiler_params=pltpu.CompilerParams(vmem_limit_bytes=VMEM_LIMIT),
        cost_estimate=pl.CostEstimate(flops=n * 45_000_000_000, bytes_accessed=n * 16 * d * ff, transcendentals=0),
        name="adamw",
    )(factor, *grads, *arrays, *old)


def ring(dim, s):
    pairs = []
    for i in range(SIDE**3):
        c = i // STRIDE[dim] % SIDE
        pairs.append((i, i + ((c + s) % SIDE - c) * STRIDE[dim]))
    return pairs


def solution(mesh):
    def step(x, dy, *arrays):
        w, m, v = (arrays[i : i + 3] for i in (0, 3, 6))
        x, dy = x[0], dy[0]
        h, p, q, act, aT, dyT = forward(x, dy, *w)
        *quarters, factor = backward(aT, dyT, dy, h, p, q, act, *w)
        second, first = quarters[0:3], quarters[3:6]

        def shift(parts, s):
            return [lax.ppermute(g, "dp", ring(k, s)) for k, g in enumerate(parts)]

        second_up, second_down = shift(second, 1), shift(second, -1)
        first_up, first_down = shift(first, 1), shift(first, -1)
        new = adamw([1, 0], [0, 0], factor, second + first, w, m, v, None)
        second_up, second_down, new = lax.optimization_barrier((second_up, second_down, new))
        second_far = shift(second_up, 1)
        new = adamw([1, 1], [-1, 1], factor, second_up + second_down, w, m, v, new)
        first_up, first_down, new = lax.optimization_barrier((first_up, first_down, new))
        first_far = shift(first_down, -1)
        new = adamw([0, 0], [-1, 1], factor, first_up + first_down, w, m, v, new)
        second_far, first_far, new = lax.optimization_barrier((second_far, first_far, new))
        new = adamw([1, 0], [2, 2], factor, second_far + first_far, w, m, v, new)
        return tuple(new)

    return jax.shard_map(
        step,
        mesh=mesh,
        in_specs=(P(("rep", "dp"), None, None),) * 2 + (P(None, None, None),) * 9,
        out_specs=(P("rep", None, None),) * 9,
        check_vma=False,
    )
```

```python
import functools

import jax
import jax.numpy as jnp
from jax import lax
from jax.experimental import pallas as pl
from jax.experimental.pallas import tpu as pltpu
from jax.sharding import PartitionSpec as P

f32, bf16 = jnp.float32, jnp.bfloat16
MESH = pl.DeviceIdType.MESH
SIDE = 4
STRIDE = (16, 4, 1)
COLS = 512
ROWS = 512
HIGH, WIDE = 48, 128
KEPT = 6
AHEAD = 4
VMEM_LIMIT = 66_900_000


def nn(a, b):
    return jnp.dot(a, b, preferred_element_type=f32)


def nt(a, b):
    return lax.dot_general(a, b, (((1,), (1,)), ((), ())), preferred_element_type=f32)


def scale_of(wide):
    return lax.rsqrt(jnp.mean(wide * wide, -1, keepdims=True) + 1e-6)


def normed(h):
    wide = h.astype(f32)
    return (wide * scale_of(wide)).astype(bf16)


def gates(gate, up):
    sig = 1.0 / (1.0 + jnp.exp(-gate))
    q = gate * sig
    return q, up * (sig + q * (1.0 - sig))


def rows_loop(tokens, body, step=256):
    def one(c, _):
        body(pl.ds(pl.multiple_of(c * step, step), step))
        return 0

    lax.fori_loop(0, tokens // step, one, 0)


def dims_of(k):
    return k, (k + 1) % 3, (k + 2) % 3


def backward_kernel(n_blocks, count, x_ref, dy_ref, wg, wu, wd, *refs):
    outs, (factor_ref, p_ref, q_ref, act_ref, aT_ref) = (refs[0:3], refs[3:6]), refs[6:11]
    (
        a_s, aT_s, dy_s, dyT_s, h_s, acc_s, wg_s, wu_s, wd_s, hidden, p_s, q_s,
        own, f1, b2, f2, b3, ag, ssq, nrm,
        through1, through2, straight1, straight2, passed1, passed2, sums2, r3,
        w_sem, in_sem, pq_sem, act_sem, keep_sem, turn_sem, own_sem,
        snd1, snd2, rcv1, rcv2, s3_snd, s3_rcv, g1_snd, g1_rcv, g2_snd, g2_rcv, n_snd, n_rcv,
    ) = refs[11:]
    tokens, d = dy_s.shape
    steps = 2 * n_blocks
    me = lax.axis_index("dp")
    at = tuple(me // s % SIDE for s in STRIDE)
    offsets = (1, 3, 2)

    def to(dim, s):
        return {"dp": me + ((at[dim] + s) % SIDE - at[dim]) * STRIDE[dim]}

    def send(src, dst, snd, rcv, dim, s):
        return pltpu.make_async_remote_copy(src_ref=src, dst_ref=dst, send_sem=snd, recv_sem=rcv, device_id=to(dim, s), device_id_type=MESH)

    barrier = pltpu.get_barrier_semaphore()
    for dim in range(3):
        for s in offsets:
            pl.semaphore_signal(barrier, inc=1, device_id=to(dim, s), device_id_type=MESH)

    def columns(i):
        return pl.ds(pl.multiple_of(i * COLS, COLS), COLS)

    def load_up(layer, i, slot):
        pairs = ((wg, wg_s), (wu, wu_s))
        return [pltpu.make_async_copy(w.at[layer, :, columns(i)], to.at[slot], w_sem.at[slot, n]) for n, (w, to) in enumerate(pairs)]

    def load_down(layer, i, slot):
        return pltpu.make_async_copy(wd.at[layer, columns(i), :], wd_s.at[slot], w_sem.at[slot, 2])

    chunks = [pl.ds(c * ROWS, ROWS) for c in range(tokens // ROWS)]

    def load_pq(i):
        pairs = ((p_ref, p_s), (q_ref, q_s))
        return [
            pltpu.make_async_copy(src.at[r, columns(i)], to.at[c], pq_sem.at[n, c])
            for n, (src, to) in enumerate(pairs)
            for c, r in enumerate(chunks)
        ]

    def load_act(i):
        return pltpu.make_async_copy(act_ref.at[:, columns(i)], hidden.at[0], act_sem)

    def keep(i, c):
        slot = (len(chunks) * i + c) % p_s.shape[0]
        pairs = ((p_s.at[slot], p_ref), (q_s.at[slot], q_ref), (hidden.at[i % 2, chunks[c]], act_ref))
        return [pltpu.make_async_copy(src, to.at[chunks[c], columns(i)], keep_sem.at[slot, n]) for n, (src, to) in enumerate(pairs)]

    def turned(i):
        return pl.ds(pl.multiple_of(i * WIDE, WIDE), WIDE)

    def keep_turned(i):
        return pltpu.make_async_copy(aT_s.at[turned(i)], aT_ref.at[turned(i)], turn_sem.at[i])

    def start(copies):
        for c in copies:
            c.start()

    def wait(copies):
        for c in copies:
            c.wait()

    load_x = pltpu.make_async_copy(x_ref, h_s, in_sem.at[0])
    load_dy = pltpu.make_async_copy(dy_ref, dy_s, in_sem.at[1])
    load_aT = pltpu.make_async_copy(aT_ref, aT_s, in_sem.at[0])
    start([load_x, *load_up(0, 0, 0), load_down(0, 0, 0), load_dy])
    ssq[...] = jnp.zeros_like(ssq)
    load_x.wait()

    def begin(r):
        a_s[r, :] = normed(h_s[r, :])
        acc_s[r, :] = jnp.zeros((r.size, d), f32)

    rows_loop(tokens, begin)
    load_dy.wait()

    def forward(i, _):
        slot = i % 2
        wait([*load_up(0, i, slot), load_down(0, i, slot)])

        @pl.when(i < n_blocks - 1)
        def _():
            start([*load_up(0, i + 1, 1 - slot), load_down(0, i + 1, 1 - slot)])

        @pl.when(i == n_blocks - 1)
        def _():
            start([*load_up(1, 0, 1 - slot), load_down(1, 0, 1 - slot)])

        for c in range(len(chunks)):

            @pl.when(len(chunks) * i + c >= p_s.shape[0])
            def _():
                before = len(chunks) * i + c - p_s.shape[0]
                for other in range(len(chunks)):
                    if (c - p_s.shape[0] - other) % len(chunks) == 0:
                        wait(keep(before // len(chunks), other))

        for c, r in enumerate(chunks):
            aT_s[turned(i), r] = a_s[r, turned(i)].T
            dyT_s[turned(i), r] = dy_s[r, turned(i)].T
            a = a_s[r, :]
            gate, up = nn(a, wg_s[slot]), nn(a, wu_s[slot])
            q, p = gates(gate, up)
            at_slot = (len(chunks) * i + c) % p_s.shape[0]
            p_s[at_slot] = p
            q_s[at_slot] = q
            act = (q * up).astype(bf16)
            hidden[slot, r, :] = act
            acc_s[r, :] += nn(act, wd_s[slot])
            start(keep(i, c))
        keep_turned(i).start()
        return 0

    lax.fori_loop(0, n_blocks, forward, 0)
    for i in range(n_blocks):
        keep_turned(i).wait()

    def add(r):
        h = (h_s[r, :].astype(f32) + acc_s[r, :].astype(bf16).astype(f32)).astype(bf16)
        h_s[r, :] = h
        a = normed(h)
        a_s[r, :] = a
        aT_s[:, r] = a.T
        acc_s[r, :] = jnp.zeros((r.size, d), f32)

    rows_loop(tokens, add)
    for last in range(n_blocks * len(chunks) - p_s.shape[0], n_blocks * len(chunks)):
        wait(keep(last // len(chunks), last % len(chunks)))
    start(load_pq(0))
    pl.semaphore_wait(barrier, 9)

    def second_layer(i):
        slot = i % 2
        wait([*load_up(1, i, slot), load_down(1, i, slot)])

        @pl.when(i < n_blocks - 1)
        def _():
            start([*load_up(1, i + 1, 1 - slot), load_down(1, i + 1, 1 - slot)])

        @pl.when(i == n_blocks - 1)
        def _():
            load_down(0, 0, 1 - slot).start()

        for r in chunks:
            a = a_s[r, :]
            gate, up = nn(a, wg_s[slot]), nn(a, wu_s[slot])
            by_act = nt(dy_s[r, :], wd_s[slot]).astype(bf16).astype(f32)
            q, p = gates(gate, up)
            hidden[0, r, :] = (q * up).astype(bf16)
            by_gate, by_up = (by_act * p).astype(bf16), (by_act * q).astype(bf16)
            hidden[1, r, :] = by_gate
            hidden[2, r, :] = by_up
            acc_s[r, :] += nt(by_gate, wg_s[slot]) + nt(by_up, wu_s[slot])

    def between():
        load_aT.start()

        def back(r):
            wide = h_s[r, :].astype(f32)
            s = scale_of(wide)
            by_a = acc_s[r, :].astype(bf16).astype(f32)
            along = jnp.sum(by_a * wide, -1, keepdims=True)
            by_h = (by_a * s - wide * (s * s * s * along * (1.0 / d))).astype(bf16)
            total = (dy_s[r, :].astype(f32) + by_h.astype(f32)).astype(bf16)
            dy_s[r, :] = total
            dyT_s[:, r] = total.T

        rows_loop(tokens, back)
        load_aT.wait()

    def first_layer(i, block):
        slot = i % 2
        load_act(block).start()
        wait([load_down(0, block, slot), *load_pq(block)])

        @pl.when(block < n_blocks - 1)
        def _():
            load_down(0, block + 1, 1 - slot).start()

        for c, r in enumerate(chunks):
            by_act = nt(dy_s[r, :], wd_s[slot]).astype(bf16).astype(f32)
            hidden[1, r, :] = (by_act * p_s[c]).astype(bf16)
            hidden[2, r, :] = (by_act * q_s[c]).astype(bf16)

        @pl.when(block < n_blocks - 1)
        def _():
            start(load_pq(block + 1))

        load_act(block).wait()

    def weight_gradient(slot, k):
        turned_s = aT_s if k < 2 else dyT_s
        g = nn(turned_s[...], hidden[(k + 1) % 3]).astype(bf16)
        for p in range(SIDE):
            for q in range(SIDE):
                for r in range(SIDE):
                    row, col = ((p * SIDE + q), r) if k < 2 else ((q * SIDE + r), p)
                    own[slot, k, p, q, r] = g[row * HIGH : row * HIGH + HIGH, col * WIDE : col * WIDE + WIDE]

    stages = (
        (through1, straight1, passed1, snd1, rcv1),
        (through2, straight2, passed2, snd2, rcv2),
    )

    def piece(stage, j, k, whose, half):
        part = pl.ds(half * 2, 2)
        return b2.at[k, whose, part] if stage else own.at[j % own.shape[0], k, whose, part]

    def around(stage, k):
        c = at[dims_of(k)[stage]]
        return (c + 1) % SIDE, (c + 3) % SIDE, (c + 2) % SIDE

    def sends(stage, kind, j, k):
        buffers, snd, rcv = stages[stage][:3], stages[stage][-2], stages[stage][-1]
        nxt, prv, far = around(stage, k)
        slot = j % buffers[kind].shape[0]
        copies = []
        for half in range(2):
            down = half == 0 if kind != 1 else half == 1
            whose = (far, (nxt, prv)[half], (prv, nxt)[half])[kind]
            src = sums2.at[k, half] if stage and kind == 2 else piece(stage, j, k, whose, half)
            copies.append(
                send(src, buffers[kind].at[slot, k, half], snd.at[kind, j % 2, k, half], rcv.at[kind, slot, k, half], dims_of(k)[stage], 3 if down else 1)
            )
        return copies

    def pass_on(stage, j):
        through = stages[stage][0]
        slot, own_slot = j % 2, j % own.shape[0]
        for k in range(3):
            nxt, prv, _ = around(stage, k)
            onward = sends(stage, 2, j, k)
            for c in sends(stage, 0, j, k):
                c.wait_recv()
            for half, whose in enumerate((prv, nxt)):
                for q in range(2):
                    if stage:
                        sums2[k, half, q] = (through[slot, k, half, q].astype(f32) + f1[slot, k, whose, half * 2 + q]).astype(bf16)
                    else:
                        for r in range(SIDE):
                            mine = own[own_slot, k, whose, half * 2 + q, r].astype(f32)
                            mine = (through[slot, k, half, q, r].astype(f32) + mine).astype(bf16)
                            own[own_slot, k, whose, half * 2 + q, r] = mine
                onward[half].start()
        if stage:
            done_sending(stage, (0, 1), j)

    def done_sending(stage, kinds, j):
        for k in range(3):
            for kind in kinds:
                for c in sends(stage, kind, j, k):
                    c.wait_send()

    def sum_1(j):
        slot, far_slot, own_slot = j % 2, j % straight1.shape[0], j % own.shape[0]
        for k in range(3):
            c = at[dims_of(k)[0]]
            for half in range(2):
                sends(0, 1, j, k)[half].wait_recv()
                sends(0, 2, j, k)[half].wait_recv()
                for q in range(2):
                    for r in range(SIDE):
                        total = own[own_slot, k, c, half * 2 + q, r].astype(f32) + passed1[slot, k, half, q, r].astype(f32)
                        total = total + straight1[far_slot, k, half, q, r].astype(f32)
                        f1[slot, k, half * 2 + q, r] = total
                        b2[k, half * 2 + q, r] = total.astype(bf16)
            start(sends(1, 0, j, k) + sends(1, 1, j, k))
        done_sending(0, range(3), j)

    def sum_2(j):
        slot, far_slot = j % 2, j % straight2.shape[0]
        for k in range(3):
            c = at[dims_of(k)[1]]
            for half in range(2):
                sends(1, 1, j, k)[half].wait_recv()
                sends(1, 2, j, k)[half].wait_recv()
                for q in range(2):
                    total = f1[slot, k, c, half * 2 + q] + passed2[slot, k, half, q].astype(f32)
                    total = total + straight2[far_slot, k, half, q].astype(f32)
                    f2[k, half * 2 + q] = total
                    b3[k, half * 2 + q] = total.astype(bf16)
            start(sends_3(slot, k))
        done_sending(1, (2,), j)

    def sends_3(slot, k):
        r = dims_of(k)[2]
        return [send(b3.at[k, (at[r] + s) % SIDE], r3.at[slot, k, s - 1], s3_snd.at[k, s - 1], s3_rcv.at[slot, k, s - 1], r, s) for s in offsets]

    def sends_g1(j, k):
        r = dims_of(k)[2]
        mine = ag.at[j, k, at[r]]
        return [send(mine, mine, g1_snd.at[j, k, s - 1], g1_rcv.at[j, k, s - 1], r, s) for s in offsets]

    def sum_3(j):
        slot = j % 2
        for k in range(3):
            for c in sends_3(slot, k):
                c.wait_recv()
            total = f2[k, at[dims_of(k)[2]]]
            for s in range(3):
                total = total + r3[slot, k, s].astype(f32)
            g = total.astype(bf16)
            ag[j, k, at[dims_of(k)[2]]] = g
            start(sends_g1(j, k))
            wide = g.astype(f32)
            wide = wide * wide
            for row in range(0, HIGH, 8):
                ssq[...] += wide[row : row + 8]
        for k in range(3):
            for c in sends_3(slot, k):
                c.wait_send()

    def by_half(j, do):
        @pl.when(j < n_blocks)
        def _():
            do(j, outs[0])

        @pl.when(j >= n_blocks)
        def _():
            do(j - n_blocks, outs[1])

    def sends_g2(j, block, out, k):
        q = dims_of(k)[1]
        mine = ag.at[j, k]
        return [send(mine, out[k].at[block, at[q]], g2_snd.at[0, j, k, way], g2_rcv.at[0, j, k, way], q, s) for way, s in enumerate((1, 3))]

    def keep_g2(j, block, out, k):
        return pltpu.make_async_copy(ag.at[j, k], out[k].at[block, at[dims_of(k)[1]]], own_sem.at[j, k])

    def sends_g3(j, block, out, k):
        q = dims_of(k)[1]
        copies = []
        for way, s in enumerate((1, 3)):
            part = out[k].at[block, (at[q] + SIDE - s) % SIDE, pl.ds(way * 2, 2)]
            copies.append(send(part, part, g2_snd.at[1, j, k, way], g2_rcv.at[1, j, k, way], q, s))
        return copies

    def share(j):
        for k in range(3):
            wait(sends_g1(j, k))

        def do(block, out):
            for k in range(3):
                start(sends_g2(j, block, out, k) + [keep_g2(j, block, out, k)])

        by_half(j, do)

    def share_on(j):
        def do(block, out):
            for k in range(3):
                for there, on in zip(sends_g2(j, block, out, k), sends_g3(j, block, out, k), strict=True):
                    there.wait_recv()
                    on.start()

        by_half(j, do)

    def shared(j):
        def do(block, out):
            for k in range(3):
                for c in sends_g2(j, block, out, k):
                    c.wait_send()
                keep_g2(j, block, out, k).wait()
                wait(sends_g3(j, block, out, k))

        by_half(j, do)

    def sends_n(stage):
        mine = nrm.at[stage, at[stage]]
        return [send(mine, mine, n_snd.at[stage, s - 1], n_rcv.at[stage, s - 1], stage, s) for s in offsets]

    def norm_send(stage, value):
        nrm[stage, at[stage]] = value
        start(sends_n(stage))

    def norm_take(stage):
        wait(sends_n(stage))
        total = nrm[stage, 0]
        for s in range(1, SIDE):
            total = total + nrm[stage, s]
        return total

    def when(i, lag, do, *args):
        pl.when((i >= lag) & (i < steps + lag))(lambda: do(*args, i - lag))

    def each(do, low, high):
        def one(j, _):
            do(j)
            return 0

        lax.fori_loop(low, high, one, 0)

    def due(i):
        return jnp.clip(2 * (i + 1 - steps), 0, steps - 2)

    def step(i, _):
        @pl.when(i < n_blocks)
        def _():
            second_layer(i)

        @pl.when(i == n_blocks)
        def _():
            between()

        @pl.when((i >= n_blocks) & (i < steps))
        def _():
            first_layer(i, i - n_blocks)

        @pl.when(i < steps)
        def _():
            weight_gradient(i % own.shape[0], 0)

        when(i, 5, sum_3)

        @pl.when(i == steps + 4)
        def _():
            norm_send(0, ssq[...])

        when(i, 4, sum_2)
        when(i, 3, pass_on, 1)
        when(i, 2, sum_1)
        when(i, 1, pass_on, 0)

        @pl.when(i < steps)
        def _():
            for k in range(3):
                if k:
                    weight_gradient(i % own.shape[0], k)
                start(sends(0, 0, i, k) + sends(0, 1, i, k))

        each(share_on, due(i - 3), due(i - 2))
        each(share, due(i - 1), due(i))
        return 0

    lax.fori_loop(0, steps + 5, step, 0)
    norm_send(1, norm_take(0))
    each(share_on, due(steps + 2), steps - 2)
    each(share, steps - 2, steps)
    norm_send(2, norm_take(1))
    each(share_on, steps - 2, steps)
    total = jnp.sum(norm_take(2), keepdims=True)
    factor = jnp.minimum(1.0, 0.5 * lax.rsqrt(total * (1.0 / count) + 1e-30))
    factor_ref[...] = jnp.broadcast_to(factor, factor_ref.shape)
    each(shared, 0, steps)


def backward(x, dy, wg, wu, wd):
    tokens, d = dy.shape
    ff = wg.shape[2]
    n_blocks = ff // COLS
    steps = 2 * n_blocks
    anywhere = pl.BlockSpec(memory_space=pl.ANY)
    shard = (HIGH, WIDE)
    quarter = jax.ShapeDtypeStruct((n_blocks, SIDE, SIDE, *shard), bf16)

    def dma(*shape):
        return pltpu.SemaphoreType.DMA(shape)

    def narrow(*shape):
        return pltpu.VMEM(shape, bf16)

    def wide(*shape):
        return pltpu.VMEM(shape, f32)

    halves1, halves2 = (3, 2, 2, SIDE, *shard), (3, 2, 2, *shard)
    return pl.pallas_call(
        functools.partial(backward_kernel, n_blocks, float(6 * d * ff)),
        out_shape=(
            *(quarter,) * 6,
            jax.ShapeDtypeStruct((8, 128), f32),
            *(jax.ShapeDtypeStruct((tokens, ff), f32),) * 2,
            jax.ShapeDtypeStruct((tokens, ff), bf16),
            jax.ShapeDtypeStruct((d, tokens), bf16),
        ),
        in_specs=[anywhere] * 5,
        out_specs=(*(anywhere,) * 6, pl.BlockSpec(memory_space=pltpu.VMEM), *(anywhere,) * 4),
        scratch_shapes=[
            *(narrow(tokens, d), narrow(d, tokens)) * 2,
            narrow(tokens, d),
            wide(tokens, d),
            *(narrow(2, d, COLS),) * 2,
            narrow(2, COLS, d),
            narrow(3, tokens, COLS),
            *(wide(KEPT, ROWS, COLS),) * 2,
            narrow(3, 3, SIDE, SIDE, SIDE, *shard),
            wide(2, 3, SIDE, SIDE, *shard),
            narrow(3, SIDE, SIDE, *shard),
            wide(3, SIDE, *shard),
            narrow(3, SIDE, *shard),
            narrow(steps, 3, SIDE, *shard),
            wide(8, 128),
            wide(3, SIDE, 8, 128),
            narrow(2, *halves1),
            narrow(2, *halves2),
            narrow(3, *halves1),
            narrow(3, *halves2),
            narrow(2, *halves1),
            narrow(2, *halves2),
            narrow(*halves2),
            narrow(2, 3, 3, *shard),
            dma(2, 3),
            dma(2),
            dma(2, tokens // ROWS),
            dma(),
            dma(KEPT, 3),
            dma(n_blocks),
            dma(steps, 3),
            *(dma(3, 2, 3, 2),) * 2,
            *(dma(3, 3, 3, 2),) * 2,
            dma(3, 3),
            dma(2, 3, 3),
            *(dma(steps, 3, 3),) * 2,
            *(dma(2, steps, 3, 2),) * 2,
            *(dma(3, 3),) * 2,
        ],
        compiler_params=pltpu.CompilerParams(vmem_limit_bytes=VMEM_LIMIT, collective_id=0, has_side_effects=True),
        cost_estimate=pl.CostEstimate(flops=30 * tokens * d * ff, bytes_accessed=20 * tokens * ff, transcendentals=0),
        name="backward",
    )(x, dy, wg, wu, wd)


def adamw_tile(factor, w, m, v, g):
    g = g.astype(f32) * factor
    m = 0.9 * m + 0.1 * g
    v = 0.95 * v + 0.05 * (g * g)
    wide = w.astype(f32)
    return (wide - 0.02 * (m * lax.rsqrt(v + 1e-8) + 0.1 * wide)).astype(bf16), m, v


def adamw_kernel(parts, shifts, n_blocks, factor_ref, *refs):
    n = len(parts)
    refs = list(refs)

    def take(count):
        taken = refs[:count]
        del refs[:count]
        return taken

    grads, arrays = take(3 * n), take(9)
    g_sem, in_sem, out_sem = refs[-3:]
    new, g_s, ins, outs = refs[-33:-24], refs[-24:-21], refs[-21:-12], refs[-12:-3]
    factor = factor_ref[...]
    me = lax.axis_index("dp")
    at = tuple(me // s % SIDE for s in STRIDE)
    steps = n * n_blocks

    def tile(k, i):
        part, block = i // n_blocks, i % n_blocks
        layer, shift = parts[0], shifts[0]
        if n > 1:
            layer, shift = layer + (parts[1] - layer) * part, shift + (shifts[1] - shift) * part
        quarter = (at[k] + shift + SIDE) % SIDE
        rows, cols = ins[k].shape[1:]
        if k < 2:
            return layer, pl.ds(pl.multiple_of(quarter * rows, rows), rows), pl.ds(pl.multiple_of(block * cols, cols), cols)
        row = pl.multiple_of((SIDE * block + quarter) * rows, rows)
        return layer, pl.ds(row, rows), slice(None)

    def loads(k, i):
        slot = i % AHEAD
        return [
            pltpu.make_async_copy(arrays[j].at[tile(k, i)], ins[j].at[slot], in_sem.at[slot, j]) for j in range(k, 9, 3)
        ]

    def load_g(k, i, part):
        slot = i % AHEAD
        return pltpu.make_async_copy(grads[3 * part + k].at[i % n_blocks], g_s[k].at[slot], g_sem.at[slot, k])

    def start(k, i):
        for c in loads(k, i):
            c.start()
        for part in range(n):

            @pl.when(i // n_blocks == part)
            def _():
                load_g(k, i, part).start()

    def stores(k, i):
        slot = i % 2
        return [
            pltpu.make_async_copy(outs[j].at[slot], new[j].at[tile(k, i)], out_sem.at[slot, j]) for j in range(k, 9, 3)
        ]

    def wait(k, i):
        for c in stores(k, i):
            c.wait()

    def first(i, _):
        for k in range(3):
            start(k, i)
        return 0

    lax.fori_loop(0, AHEAD, first, 0)

    def step(i, _):
        slot, out = i % AHEAD, i % 2
        for k in range(3):
            for c in loads(k, i):
                c.wait()
            load_g(k, i, 0).wait()

            @pl.when(i >= 2)
            def _():
                wait(k, i - 2)

            def one(where, g):
                done = adamw_tile(factor[0:1, 0:1], *(ins[j][(slot, *where)] for j in range(k, 9, 3)), g)
                for j, value in zip(range(k, 9, 3), done, strict=True):
                    outs[j][(out, *where)] = value

            if k < 2:
                for q in range(SIDE):
                    for r in range(SIDE):
                        one((pl.ds(q * HIGH, HIGH), pl.ds(r * WIDE, WIDE)), g_s[k][slot, q, r])
            else:
                for lo in range(0, SIDE * SIDE * HIGH, WIDE):
                    pieces = [divmod(e, HIGH) for e in range(lo, lo + WIDE, 16)]
                    rows = [g_s[k][slot, n // SIDE, n % SIDE, pl.ds(row, 16)] for n, row in pieces]
                    one((slice(None), pl.ds(lo, WIDE)), jnp.concatenate(rows, 0).T)
            for c in stores(k, i):
                c.start()

            @pl.when(i + AHEAD < steps)
            def _():
                start(k, i + AHEAD)

        return 0

    lax.fori_loop(0, steps, step, 0)
    for k in range(3):
        wait(k, steps - 2)
        wait(k, steps - 1)


def adamw(parts, shifts, factor, grads, w, m, v, into):
    n, n_blocks = len(parts), grads[0].shape[0]
    d, ff = w[0].shape[1:]
    arrays = list(w) + list(m) + list(v)
    anywhere = pl.BlockSpec(memory_space=pl.ANY)
    tiles = [(d // SIDE, COLS), (d // SIDE, COLS), (COLS // SIDE, d)] * 3
    old = list(into or [])
    return pl.pallas_call(
        functools.partial(adamw_kernel, parts, shifts, n_blocks),
        out_shape=tuple(jax.ShapeDtypeStruct(a.shape, a.dtype) for a in arrays),
        in_specs=[pl.BlockSpec(memory_space=pltpu.VMEM)] + [anywhere] * (len(grads) + 9 + len(old)),
        out_specs=(anywhere,) * 9,
        input_output_aliases={1 + len(grads) + 9 + j: j for j in range(len(old))},
        scratch_shapes=[pltpu.VMEM((AHEAD, *grads[0].shape[1:]), bf16)] * 3
        + [pltpu.VMEM((AHEAD, *t), a.dtype) for t, a in zip(tiles, arrays, strict=True)]
        + [pltpu.VMEM((2, *t), a.dtype) for t, a in zip(tiles, arrays, strict=True)]
        + [pltpu.SemaphoreType.DMA(s) for s in ((AHEAD, 3), (AHEAD, 9), (2, 9))],
        compiler_params=pltpu.CompilerParams(vmem_limit_bytes=VMEM_LIMIT),
        cost_estimate=pl.CostEstimate(flops=n * 45_000_000_000, bytes_accessed=n * 16 * d * ff, transcendentals=0),
        name="adamw",
    )(factor, *grads, *arrays, *old)


def ring(dim, s):
    pairs = []
    for i in range(SIDE**3):
        c = i // STRIDE[dim] % SIDE
        pairs.append((i, i + ((c + s) % SIDE - c) * STRIDE[dim]))
    return pairs


def solution(mesh):
    def step(x, dy, *arrays):
        w, m, v = (arrays[i : i + 3] for i in (0, 3, 6))
        x, dy = x[0], dy[0]
        results = backward(x, dy, *w)
        second, first, factor = results[0:3], results[3:6], results[6]

        def shift(parts, s):
            return [lax.ppermute(g, "dp", ring(k, s)) for k, g in enumerate(parts)]

        second_up, second_down = shift(second, 1), shift(second, -1)
        first_up, first_down = shift(first, 1), shift(first, -1)
        new = adamw([1, 0], [0, 0], factor, second + first, w, m, v, None)
        second_up, second_down, new = lax.optimization_barrier((second_up, second_down, new))
        second_far = shift(second_up, 1)
        new = adamw([1, 1], [-1, 1], factor, second_up + second_down, w, m, v, new)
        first_up, first_down, new = lax.optimization_barrier((first_up, first_down, new))
        first_far = shift(first_down, -1)
        new = adamw([0, 0], [-1, 1], factor, first_up + first_down, w, m, v, new)
        second_far, first_far, new = lax.optimization_barrier((second_far, first_far, new))
        new = adamw([1, 0], [2, 2], factor, second_far + first_far, w, m, v, new)
        return tuple(new)

    return jax.shard_map(
        step,
        mesh=mesh,
        in_specs=(P(("rep", "dp"), None, None),) * 2 + (P(None, None, None),) * 9,
        out_specs=(P("rep", None, None),) * 9,
        check_vma=False,
    )
```

```python
import functools

import jax
import jax.numpy as jnp
from jax import lax
from jax.experimental import pallas as pl
from jax.experimental.pallas import tpu as pltpu
from jax.sharding import PartitionSpec as P

f32, bf16 = jnp.float32, jnp.bfloat16
MESH = pl.DeviceIdType.MESH
SIDE = 4
STRIDE = (16, 4, 1)
COLS = 512
ROWS = 512
HIGH, WIDE = 48, 128
KEPT = 5
AHEAD = 4
VMEM_LIMIT = 66_900_000


def nn(a, b):
    return jnp.dot(a, b, preferred_element_type=f32)


def nt(a, b):
    return lax.dot_general(a, b, (((1,), (1,)), ((), ())), preferred_element_type=f32)


def scale_of(wide):
    return lax.rsqrt(jnp.mean(wide * wide, -1, keepdims=True) + 1e-6)


def normed(h):
    wide = h.astype(f32)
    return (wide * scale_of(wide)).astype(bf16)


def gates(gate, up):
    sig = 1.0 / (1.0 + jnp.exp(-gate))
    q = gate * sig
    return q, up * (sig + q * (1.0 - sig))


def rows_loop(tokens, body, step=256):
    def one(c, _):
        body(pl.ds(pl.multiple_of(c * step, step), step))
        return 0

    lax.fori_loop(0, tokens // step, one, 0)


def dims_of(k):
    return k, (k + 1) % 3, (k + 2) % 3


def backward_kernel(n_blocks, count, x_ref, dy_ref, wg, wu, wd, *refs):
    outs, (factor_ref, p_ref, q_ref, act_ref, aT_ref) = (refs[0:3], refs[3:6]), refs[6:11]
    (
        a_s, aT_s, dy_s, dyT_s, h_s, acc_s, wg_s, wu_s, wd_s, hidden, p_s, q_s,
        own, f1, b2, f2, b3, ag, ssq, nrm,
        through1, through2, straight1, straight2, passed1, passed2, sums2, r3,
        w_sem, in_sem, pq_sem, act_sem, keep_sem, turn_sem, own_sem,
        snd1, snd2, rcv1, rcv2, s3_snd, s3_rcv, g1_snd, g1_rcv, g2_snd, g2_rcv, n_snd, n_rcv,
    ) = refs[11:]
    tokens, d = dy_s.shape
    steps = 2 * n_blocks
    me = lax.axis_index("dp")
    at = tuple(me // s % SIDE for s in STRIDE)
    offsets = (1, 3, 2)

    def to(dim, s):
        return {"dp": me + ((at[dim] + s) % SIDE - at[dim]) * STRIDE[dim]}

    def send(src, dst, snd, rcv, dim, s):
        return pltpu.make_async_remote_copy(src_ref=src, dst_ref=dst, send_sem=snd, recv_sem=rcv, device_id=to(dim, s), device_id_type=MESH)

    barrier = pltpu.get_barrier_semaphore()
    for dim in range(3):
        for s in offsets:
            pl.semaphore_signal(barrier, inc=1, device_id=to(dim, s), device_id_type=MESH)

    def columns(i):
        return pl.ds(pl.multiple_of(i * COLS, COLS), COLS)

    def load_up(layer, i, slot):
        pairs = ((wg, wg_s), (wu, wu_s))
        return [pltpu.make_async_copy(w.at[layer, :, columns(i)], to.at[slot], w_sem.at[slot, n]) for n, (w, to) in enumerate(pairs)]

    def load_down(layer, i, slot):
        return pltpu.make_async_copy(wd.at[layer, columns(i), :], wd_s.at[slot], w_sem.at[slot, 2])

    chunks = [pl.ds(c * ROWS, ROWS) for c in range(tokens // ROWS)]

    def load_pq(i):
        pairs = ((p_ref, p_s), (q_ref, q_s))
        return [
            pltpu.make_async_copy(src.at[r, columns(i)], to.at[c], pq_sem.at[n, c])
            for n, (src, to) in enumerate(pairs)
            for c, r in enumerate(chunks)
        ]

    def load_act(i):
        return pltpu.make_async_copy(act_ref.at[:, columns(i)], hidden.at[0], act_sem)

    def keep(i, c):
        slot = (len(chunks) * i + c) % p_s.shape[0]
        pairs = ((p_s.at[slot], p_ref), (q_s.at[slot], q_ref), (hidden.at[i % 2, chunks[c]], act_ref))
        return [pltpu.make_async_copy(src, to.at[chunks[c], columns(i)], keep_sem.at[slot, n]) for n, (src, to) in enumerate(pairs)]

    def turned(i):
        return pl.ds(pl.multiple_of(i * WIDE, WIDE), WIDE)

    def keep_turned(i):
        return pltpu.make_async_copy(aT_s.at[turned(i)], aT_ref.at[turned(i)], turn_sem.at[i])

    def start(copies):
        for c in copies:
            c.start()

    def wait(copies):
        for c in copies:
            c.wait()

    load_x = pltpu.make_async_copy(x_ref, h_s, in_sem.at[0])
    load_dy = pltpu.make_async_copy(dy_ref, dy_s, in_sem.at[1])
    load_aT = pltpu.make_async_copy(aT_ref, aT_s, in_sem.at[0])
    start([load_x, *load_up(0, 0, 0), load_down(0, 0, 0), load_dy])
    ssq[...] = jnp.zeros_like(ssq)
    load_x.wait()

    def begin(r):
        a_s[r, :] = normed(h_s[r, :])
        acc_s[r, :] = jnp.zeros((r.size, d), f32)

    rows_loop(tokens, begin)
    load_dy.wait()

    def forward(i, _):
        slot = i % 2
        wait([*load_up(0, i, slot), load_down(0, i, slot)])

        @pl.when(i < n_blocks - 1)
        def _():
            start([*load_up(0, i + 1, 1 - slot), load_down(0, i + 1, 1 - slot)])

        @pl.when(i == n_blocks - 1)
        def _():
            start([*load_up(1, 0, 1 - slot), load_down(1, 0, 1 - slot)])

        for c in range(len(chunks)):

            @pl.when(len(chunks) * i + c >= p_s.shape[0])
            def _():
                before = len(chunks) * i + c - p_s.shape[0]
                for other in range(len(chunks)):
                    if (c - p_s.shape[0] - other) % len(chunks) == 0:
                        wait(keep(before // len(chunks), other))

        for c, r in enumerate(chunks):
            aT_s[turned(i), r] = a_s[r, turned(i)].T
            dyT_s[turned(i), r] = dy_s[r, turned(i)].T
            a = a_s[r, :]
            gate, up = nn(a, wg_s[slot]), nn(a, wu_s[slot])
            q, p = gates(gate, up)
            at_slot = (len(chunks) * i + c) % p_s.shape[0]
            p_s[at_slot] = p
            q_s[at_slot] = q
            act = (q * up).astype(bf16)
            hidden[slot, r, :] = act
            acc_s[r, :] += nn(act, wd_s[slot])
            start(keep(i, c))
        keep_turned(i).start()
        return 0

    lax.fori_loop(0, n_blocks, forward, 0)
    for i in range(n_blocks):
        keep_turned(i).wait()

    def add(r):
        h = (h_s[r, :].astype(f32) + acc_s[r, :].astype(bf16).astype(f32)).astype(bf16)
        h_s[r, :] = h
        a = normed(h)
        a_s[r, :] = a
        aT_s[:, r] = a.T
        acc_s[r, :] = jnp.zeros((r.size, d), f32)

    rows_loop(tokens, add)
    for last in range(n_blocks * len(chunks) - p_s.shape[0], n_blocks * len(chunks)):
        wait(keep(last // len(chunks), last % len(chunks)))
    start(load_pq(0))
    pl.semaphore_wait(barrier, 9)

    def second_layer(i):
        slot = i % 2
        wait([*load_up(1, i, slot), load_down(1, i, slot)])

        @pl.when(i < n_blocks - 1)
        def _():
            start([*load_up(1, i + 1, 1 - slot), load_down(1, i + 1, 1 - slot)])

        @pl.when(i == n_blocks - 1)
        def _():
            load_down(0, 0, 1 - slot).start()

        def finish(r, gate, up, by_act):
            q, p = gates(gate, up)
            hidden[0, r, :] = (q * up).astype(bf16)
            by_gate, by_up = (by_act * p).astype(bf16), (by_act * q).astype(bf16)
            hidden[1, r, :] = by_gate
            hidden[2, r, :] = by_up
            acc_s[r, :] += nt(by_gate, wg_s[slot]) + nt(by_up, wu_s[slot])

        ready = None
        for r in [pl.ds(lo, ROWS // 2) for lo in range(0, tokens, ROWS // 2)]:
            a = a_s[r, :]
            gate, up = nn(a, wg_s[slot]), nn(a, wu_s[slot])
            by_act = nt(dy_s[r, :], wd_s[slot]).astype(bf16).astype(f32)
            if ready:
                finish(*ready)
            ready = r, gate, up, by_act
        finish(*ready)

    def between():
        load_aT.start()

        def back(r):
            wide = h_s[r, :].astype(f32)
            s = scale_of(wide)
            by_a = acc_s[r, :].astype(bf16).astype(f32)
            along = jnp.sum(by_a * wide, -1, keepdims=True)
            by_h = (by_a * s - wide * (s * s * s * along * (1.0 / d))).astype(bf16)
            total = (dy_s[r, :].astype(f32) + by_h.astype(f32)).astype(bf16)
            dy_s[r, :] = total
            dyT_s[:, r] = total.T

        rows_loop(tokens, back)
        load_aT.wait()

    def first_layer(i, block):
        slot = i % 2
        load_act(block).start()
        wait([load_down(0, block, slot), *load_pq(block)])

        @pl.when(block < n_blocks - 1)
        def _():
            load_down(0, block + 1, 1 - slot).start()

        for c, r in enumerate(chunks):
            by_act = nt(dy_s[r, :], wd_s[slot]).astype(bf16).astype(f32)
            hidden[1, r, :] = (by_act * p_s[c]).astype(bf16)
            hidden[2, r, :] = (by_act * q_s[c]).astype(bf16)

        @pl.when(block < n_blocks - 1)
        def _():
            start(load_pq(block + 1))

        load_act(block).wait()

    def weight_gradient(slot, k):
        turned_s = aT_s if k < 2 else dyT_s
        g = nn(turned_s[...], hidden[(k + 1) % 3]).astype(bf16)
        for p in range(SIDE):
            for q in range(SIDE):
                for r in range(SIDE):
                    row, col = ((p * SIDE + q), r) if k < 2 else ((q * SIDE + r), p)
                    own[slot, k, p, q, r] = g[row * HIGH : row * HIGH + HIGH, col * WIDE : col * WIDE + WIDE]

    stages = (
        (through1, straight1, passed1, snd1, rcv1),
        (through2, straight2, passed2, snd2, rcv2),
    )

    def piece(stage, j, k, whose, half):
        part = pl.ds(half * 2, 2)
        return b2.at[k, whose, part] if stage else own.at[j % own.shape[0], k, whose, part]

    def around(stage, k):
        c = at[dims_of(k)[stage]]
        return (c + 1) % SIDE, (c + 3) % SIDE, (c + 2) % SIDE

    def sends(stage, kind, j, k):
        buffers, snd, rcv = stages[stage][:3], stages[stage][-2], stages[stage][-1]
        nxt, prv, far = around(stage, k)
        slot = j % buffers[kind].shape[0]
        copies = []
        for half in range(2):
            down = half == 0 if kind != 1 else half == 1
            whose = (far, (nxt, prv)[half], (prv, nxt)[half])[kind]
            src = sums2.at[k, half] if stage and kind == 2 else piece(stage, j, k, whose, half)
            copies.append(
                send(src, buffers[kind].at[slot, k, half], snd.at[kind, j % 2, k, half], rcv.at[kind, slot, k, half], dims_of(k)[stage], 3 if down else 1)
            )
        return copies

    def pass_on(stage, j):
        through = stages[stage][0]
        slot, own_slot = j % 2, j % own.shape[0]
        for k in range(3):
            nxt, prv, _ = around(stage, k)
            onward = sends(stage, 2, j, k)
            for c in sends(stage, 0, j, k):
                c.wait_recv()
            for half, whose in enumerate((prv, nxt)):
                for q in range(2):
                    if stage:
                        sums2[k, half, q] = (through[slot, k, half, q].astype(f32) + f1[slot, k, whose, half * 2 + q]).astype(bf16)
                    else:
                        for r in range(SIDE):
                            mine = own[own_slot, k, whose, half * 2 + q, r].astype(f32)
                            mine = (through[slot, k, half, q, r].astype(f32) + mine).astype(bf16)
                            own[own_slot, k, whose, half * 2 + q, r] = mine
                onward[half].start()
        if stage:
            done_sending(stage, (0, 1), j)

    def done_sending(stage, kinds, j):
        for k in range(3):
            for kind in kinds:
                for c in sends(stage, kind, j, k):
                    c.wait_send()

    def sum_1(j):
        slot, far_slot, own_slot = j % 2, j % straight1.shape[0], j % own.shape[0]
        for k in range(3):
            c = at[dims_of(k)[0]]
            for half in range(2):
                sends(0, 1, j, k)[half].wait_recv()
                sends(0, 2, j, k)[half].wait_recv()
                for q in range(2):
                    for r in range(SIDE):
                        total = own[own_slot, k, c, half * 2 + q, r].astype(f32) + passed1[slot, k, half, q, r].astype(f32)
                        total = total + straight1[far_slot, k, half, q, r].astype(f32)
                        f1[slot, k, half * 2 + q, r] = total
                        b2[k, half * 2 + q, r] = total.astype(bf16)
            start(sends(1, 0, j, k) + sends(1, 1, j, k))
        done_sending(0, range(3), j)

    def sum_2(j):
        slot, far_slot = j % 2, j % straight2.shape[0]
        for k in range(3):
            c = at[dims_of(k)[1]]

            def together(half, q, piece):
                total = f1[slot, k, c, piece] + passed2[slot, k, half, q].astype(f32)
                return total + straight2[far_slot, k, half, q].astype(f32)

            for half in range(2):
                sends(1, 1, j, k)[half].wait_recv()
                sends(1, 2, j, k)[half].wait_recv()
                for q in range(2):
                    b3[k, half * 2 + q] = together(half, q, half * 2 + q).astype(bf16)
            mine = at[dims_of(k)[2]]
            f2[k] = together(mine // 2, mine % 2, mine)
            start(sends_3(slot, k))
        done_sending(1, (2,), j)

    def sends_3(slot, k):
        r = dims_of(k)[2]
        return [send(b3.at[k, (at[r] + s) % SIDE], r3.at[slot, k, s - 1], s3_snd.at[k, s - 1], s3_rcv.at[slot, k, s - 1], r, s) for s in offsets]

    def sends_g1(j, k):
        r = dims_of(k)[2]
        mine = ag.at[j, k, at[r]]
        return [send(mine, mine, g1_snd.at[j, k, s - 1], g1_rcv.at[j, k, s - 1], r, s) for s in offsets]

    def sum_3(j):
        slot = j % 2
        for k in range(3):
            for c in sends_3(slot, k):
                c.wait_recv()
            total = f2[k]
            for s in range(3):
                total = total + r3[slot, k, s].astype(f32)
            g = total.astype(bf16)
            ag[j, k, at[dims_of(k)[2]]] = g
            start(sends_g1(j, k))
            wide = g.astype(f32)
            wide = wide * wide
            for row in range(0, HIGH, 8):
                ssq[...] += wide[row : row + 8]
        for k in range(3):
            for c in sends_3(slot, k):
                c.wait_send()

    def by_half(j, do):
        @pl.when(j < n_blocks)
        def _():
            do(j, outs[0])

        @pl.when(j >= n_blocks)
        def _():
            do(j - n_blocks, outs[1])

    def sends_g2(j, block, out, k):
        q = dims_of(k)[1]
        mine = ag.at[j, k]
        return [send(mine, out[k].at[block, at[q]], g2_snd.at[0, j, k, way], g2_rcv.at[0, j, k, way], q, s) for way, s in enumerate((1, 3))]

    def keep_g2(j, block, out, k):
        return pltpu.make_async_copy(ag.at[j, k], out[k].at[block, at[dims_of(k)[1]]], own_sem.at[j, k])

    def sends_g3(j, block, out, k):
        q = dims_of(k)[1]
        copies = []
        for way, s in enumerate((1, 3)):
            part = out[k].at[block, (at[q] + SIDE - s) % SIDE, pl.ds(way * 2, 2)]
            copies.append(send(part, part, g2_snd.at[1, j, k, way], g2_rcv.at[1, j, k, way], q, s))
        return copies

    def share(j):
        for k in range(3):
            wait(sends_g1(j, k))

        def do(block, out):
            for k in range(3):
                start(sends_g2(j, block, out, k) + [keep_g2(j, block, out, k)])

        by_half(j, do)

    def share_on(j):
        def do(block, out):
            for k in range(3):
                for there, on in zip(sends_g2(j, block, out, k), sends_g3(j, block, out, k), strict=True):
                    there.wait_recv()
                    on.start()

        by_half(j, do)

    def shared(j):
        def do(block, out):
            for k in range(3):
                for c in sends_g2(j, block, out, k):
                    c.wait_send()
                keep_g2(j, block, out, k).wait()
                wait(sends_g3(j, block, out, k))

        by_half(j, do)

    def sends_n(stage):
        mine = nrm.at[stage, at[stage]]
        return [send(mine, mine, n_snd.at[stage, s - 1], n_rcv.at[stage, s - 1], stage, s) for s in offsets]

    def norm_send(stage, value):
        nrm[stage, at[stage]] = value
        start(sends_n(stage))

    def norm_take(stage):
        wait(sends_n(stage))
        total = nrm[stage, 0]
        for s in range(1, SIDE):
            total = total + nrm[stage, s]
        return total

    def when(i, lag, do, *args):
        pl.when((i >= lag) & (i < steps + lag))(lambda: do(*args, i - lag))

    def each(do, low, high):
        def one(j, _):
            do(j)
            return 0

        lax.fori_loop(low, high, one, 0)

    def due(i):
        return jnp.clip(2 * (i + 1 - steps), 0, steps - 2)

    def step(i, _):
        @pl.when(i < n_blocks)
        def _():
            second_layer(i)

        @pl.when(i == n_blocks)
        def _():
            between()

        @pl.when((i >= n_blocks) & (i < steps))
        def _():
            first_layer(i, i - n_blocks)

        @pl.when(i < steps)
        def _():
            weight_gradient(i % own.shape[0], 0)

        when(i, 5, sum_3)

        @pl.when(i == steps + 4)
        def _():
            norm_send(0, ssq[...])

        when(i, 4, sum_2)
        when(i, 3, pass_on, 1)
        when(i, 2, sum_1)
        when(i, 1, pass_on, 0)

        @pl.when(i < steps)
        def _():
            for k in range(3):
                if k:
                    weight_gradient(i % own.shape[0], k)
                start(sends(0, 0, i, k) + sends(0, 1, i, k))

        each(share_on, due(i - 3), due(i - 2))
        each(share, due(i - 1), due(i))
        return 0

    lax.fori_loop(0, steps + 5, step, 0)
    norm_send(1, norm_take(0))
    each(share_on, due(steps + 2), steps - 2)
    each(share, steps - 2, steps)
    norm_send(2, norm_take(1))
    each(share_on, steps - 2, steps)
    total = jnp.sum(norm_take(2), keepdims=True)
    factor = jnp.minimum(1.0, 0.5 * lax.rsqrt(total * (1.0 / count) + 1e-30))
    factor_ref[...] = jnp.broadcast_to(factor, factor_ref.shape)
    each(shared, 0, steps)


def backward(x, dy, wg, wu, wd):
    tokens, d = dy.shape
    ff = wg.shape[2]
    n_blocks = ff // COLS
    steps = 2 * n_blocks
    anywhere = pl.BlockSpec(memory_space=pl.ANY)
    shard = (HIGH, WIDE)
    quarter = jax.ShapeDtypeStruct((n_blocks, SIDE, SIDE, *shard), bf16)

    def dma(*shape):
        return pltpu.SemaphoreType.DMA(shape)

    def narrow(*shape):
        return pltpu.VMEM(shape, bf16)

    def wide(*shape):
        return pltpu.VMEM(shape, f32)

    halves1, halves2 = (3, 2, 2, SIDE, *shard), (3, 2, 2, *shard)
    return pl.pallas_call(
        functools.partial(backward_kernel, n_blocks, float(6 * d * ff)),
        out_shape=(
            *(quarter,) * 6,
            jax.ShapeDtypeStruct((8, 128), f32),
            *(jax.ShapeDtypeStruct((tokens, ff), f32),) * 2,
            jax.ShapeDtypeStruct((tokens, ff), bf16),
            jax.ShapeDtypeStruct((d, tokens), bf16),
        ),
        in_specs=[anywhere] * 5,
        out_specs=(*(anywhere,) * 6, pl.BlockSpec(memory_space=pltpu.VMEM), *(anywhere,) * 4),
        scratch_shapes=[
            *(narrow(tokens, d), narrow(d, tokens)) * 2,
            narrow(tokens, d),
            wide(tokens, d),
            *(narrow(2, d, COLS),) * 2,
            narrow(2, COLS, d),
            narrow(3, tokens, COLS),
            *(wide(KEPT, ROWS, COLS),) * 2,
            narrow(3, 3, SIDE, SIDE, SIDE, *shard),
            wide(2, 3, SIDE, SIDE, *shard),
            narrow(3, SIDE, SIDE, *shard),
            wide(3, *shard),
            narrow(3, SIDE, *shard),
            narrow(steps, 3, SIDE, *shard),
            wide(8, 128),
            wide(3, SIDE, 8, 128),
            narrow(2, *halves1),
            narrow(2, *halves2),
            narrow(3, *halves1),
            narrow(3, *halves2),
            narrow(2, *halves1),
            narrow(2, *halves2),
            narrow(*halves2),
            narrow(2, 3, 3, *shard),
            dma(2, 3),
            dma(2),
            dma(2, tokens // ROWS),
            dma(),
            dma(KEPT, 3),
            dma(n_blocks),
            dma(steps, 3),
            *(dma(3, 2, 3, 2),) * 2,
            *(dma(3, 3, 3, 2),) * 2,
            dma(3, 3),
            dma(2, 3, 3),
            *(dma(steps, 3, 3),) * 2,
            *(dma(2, steps, 3, 2),) * 2,
            *(dma(3, 3),) * 2,
        ],
        compiler_params=pltpu.CompilerParams(vmem_limit_bytes=VMEM_LIMIT, collective_id=0, has_side_effects=True),
        cost_estimate=pl.CostEstimate(flops=30 * tokens * d * ff, bytes_accessed=20 * tokens * ff, transcendentals=0),
        name="backward",
    )(x, dy, wg, wu, wd)


def adamw_tile(factor, w, m, v, g):
    g = g.astype(f32) * factor
    m = 0.9 * m + 0.1 * g
    v = 0.95 * v + 0.05 * (g * g)
    wide = w.astype(f32)
    return (wide - 0.02 * (m * lax.rsqrt(v + 1e-8) + 0.1 * wide)).astype(bf16), m, v


def adamw_kernel(parts, shifts, n_blocks, factor_ref, *refs):
    n = len(parts)
    refs = list(refs)

    def take(count):
        taken = refs[:count]
        del refs[:count]
        return taken

    grads, arrays = take(3 * n), take(9)
    g_sem, in_sem, out_sem = refs[-3:]
    new, g_s, ins, outs = refs[-33:-24], refs[-24:-21], refs[-21:-12], refs[-12:-3]
    factor = factor_ref[...]
    me = lax.axis_index("dp")
    at = tuple(me // s % SIDE for s in STRIDE)
    steps = n * n_blocks

    def tile(k, i):
        part, block = i // n_blocks, i % n_blocks
        layer, shift = parts[0], shifts[0]
        if n > 1:
            layer, shift = layer + (parts[1] - layer) * part, shift + (shifts[1] - shift) * part
        quarter = (at[k] + shift + SIDE) % SIDE
        rows, cols = ins[k].shape[1:]
        if k < 2:
            return layer, pl.ds(pl.multiple_of(quarter * rows, rows), rows), pl.ds(pl.multiple_of(block * cols, cols), cols)
        row = pl.multiple_of((SIDE * block + quarter) * rows, rows)
        return layer, pl.ds(row, rows), slice(None)

    def loads(k, i):
        slot = i % AHEAD
        return [
            pltpu.make_async_copy(arrays[j].at[tile(k, i)], ins[j].at[slot], in_sem.at[slot, j]) for j in range(k, 9, 3)
        ]

    def load_g(k, i, part):
        slot = i % AHEAD
        return pltpu.make_async_copy(grads[3 * part + k].at[i % n_blocks], g_s[k].at[slot], g_sem.at[slot, k])

    def start(k, i):
        for c in loads(k, i):
            c.start()
        for part in range(n):

            @pl.when(i // n_blocks == part)
            def _():
                load_g(k, i, part).start()

    def stores(k, i):
        slot = i % 2
        return [
            pltpu.make_async_copy(outs[j].at[slot], new[j].at[tile(k, i)], out_sem.at[slot, j]) for j in range(k, 9, 3)
        ]

    def wait(k, i):
        for c in stores(k, i):
            c.wait()

    def first(i, _):
        for k in range(3):
            start(k, i)
        return 0

    lax.fori_loop(0, AHEAD, first, 0)

    def step(i, _):
        slot, out = i % AHEAD, i % 2
        for k in range(3):
            for c in loads(k, i):
                c.wait()
            load_g(k, i, 0).wait()

            @pl.when(i >= 2)
            def _():
                wait(k, i - 2)

            def one(where, g):
                done = adamw_tile(factor[0:1, 0:1], *(ins[j][(slot, *where)] for j in range(k, 9, 3)), g)
                for j, value in zip(range(k, 9, 3), done, strict=True):
                    outs[j][(out, *where)] = value

            if k < 2:
                for q in range(SIDE):
                    for r in range(SIDE):
                        one((pl.ds(q * HIGH, HIGH), pl.ds(r * WIDE, WIDE)), g_s[k][slot, q, r])
            else:
                for lo in range(0, SIDE * SIDE * HIGH, WIDE):
                    pieces = [divmod(e, HIGH) for e in range(lo, lo + WIDE, 16)]
                    rows = [g_s[k][slot, n // SIDE, n % SIDE, pl.ds(row, 16)] for n, row in pieces]
                    one((slice(None), pl.ds(lo, WIDE)), jnp.concatenate(rows, 0).T)
            for c in stores(k, i):
                c.start()

            @pl.when(i + AHEAD < steps)
            def _():
                start(k, i + AHEAD)

        return 0

    lax.fori_loop(0, steps, step, 0)
    for k in range(3):
        wait(k, steps - 2)
        wait(k, steps - 1)


def adamw(parts, shifts, factor, grads, w, m, v, into):
    n, n_blocks = len(parts), grads[0].shape[0]
    d, ff = w[0].shape[1:]
    arrays = list(w) + list(m) + list(v)
    anywhere = pl.BlockSpec(memory_space=pl.ANY)
    tiles = [(d // SIDE, COLS), (d // SIDE, COLS), (COLS // SIDE, d)] * 3
    old = list(into or [])
    return pl.pallas_call(
        functools.partial(adamw_kernel, parts, shifts, n_blocks),
        out_shape=tuple(jax.ShapeDtypeStruct(a.shape, a.dtype) for a in arrays),
        in_specs=[pl.BlockSpec(memory_space=pltpu.VMEM)] + [anywhere] * (len(grads) + 9 + len(old)),
        out_specs=(anywhere,) * 9,
        input_output_aliases={1 + len(grads) + 9 + j: j for j in range(len(old))},
        scratch_shapes=[pltpu.VMEM((AHEAD, *grads[0].shape[1:]), bf16)] * 3
        + [pltpu.VMEM((AHEAD, *t), a.dtype) for t, a in zip(tiles, arrays, strict=True)]
        + [pltpu.VMEM((2, *t), a.dtype) for t, a in zip(tiles, arrays, strict=True)]
        + [pltpu.SemaphoreType.DMA(s) for s in ((AHEAD, 3), (AHEAD, 9), (2, 9))],
        compiler_params=pltpu.CompilerParams(vmem_limit_bytes=VMEM_LIMIT),
        cost_estimate=pl.CostEstimate(flops=n * 45_000_000_000, bytes_accessed=n * 16 * d * ff, transcendentals=0),
        name="adamw",
    )(factor, *grads, *arrays, *old)


def ring(dim, s):
    pairs = []
    for i in range(SIDE**3):
        c = i // STRIDE[dim] % SIDE
        pairs.append((i, i + ((c + s) % SIDE - c) * STRIDE[dim]))
    return pairs


def solution(mesh):
    def step(x, dy, *arrays):
        w, m, v = (arrays[i : i + 3] for i in (0, 3, 6))
        x, dy = x[0], dy[0]
        results = backward(x, dy, *w)
        second, first, factor = results[0:3], results[3:6], results[6]

        def shift(parts, s):
            return [lax.ppermute(g, "dp", ring(k, s)) for k, g in enumerate(parts)]

        second_up, first_up = shift(second, 1), shift(first, 1)
        second_again, first_again = lax.optimization_barrier((second, first))
        second_down, first_down = shift(second_again, -1), shift(first_again, -1)

        new = adamw([1, 0], [0, 0], factor, [*second, *first], w, m, v, None)
        second_up, second_down, new = lax.optimization_barrier((second_up, second_down, new))
        second_far = shift(second_up, 1)
        new = adamw([1, 1], [-1, 1], factor, [*second_up, *second_down], w, m, v, new)
        first_up, first_down, new = lax.optimization_barrier((first_up, first_down, new))
        first_far = shift(first_up, 1)
        new = adamw([0, 0], [-1, 1], factor, [*first_up, *first_down], w, m, v, new)
        second_far, new = lax.optimization_barrier((second_far, new))
        new = adamw([1], [2], factor, second_far, w, m, v, new)
        first_far, new = lax.optimization_barrier((first_far, new))
        new = adamw([0], [2], factor, first_far, w, m, v, new)
        return tuple(new)

    return jax.shard_map(
        step,
        mesh=mesh,
        in_specs=(P(("rep", "dp"), None, None),) * 2 + (P(None, None, None),) * 9,
        out_specs=(P("rep", None, None),) * 9,
        check_vma=False,
    )
```
